32 devices in a mesh: mem: 8 (over z, x), chan: 4 (over y, core).
Axes of the slice: x: 2, y: 2, z: 4, core: 2. Of those that a mesh axis runs over, the one named last changes fastest.
Arguments:
- state_anom: bfloat16 [8, 64, 137], P(None, 'mem'), may hold values from -6 to 6
- radiance_anom: bfloat16 [8, 64, 8704], P(None, 'mem', 'chan'), may hold values from -6 to 6
- inv_noise: float32 [8704], P('chan'), may hold values from 0.02 to 0.2
- innovation: float32 [8, 8704], P(None, 'chan'), may hold values from -6 to 6
- valid_count: int32 [8], replicated, may hold values from 4352 to 8461
Outputs:
- information: float32 [8, 137, 137], P('mem')
- gradient: float32 [8, 137], P('mem')
- increment: float32 [8, 137], P('mem')
The draws below stay inside these ranges and needn't reach their ends.
All inputs are finite; a program needn't handle non-finite values.
Results may differ from the reference program's by a relative error of at most 0.0003.
Values may be sent and summed in bfloat16 or wider, within the bound.
A program may use at most 64 MiB of HBM per device.

```python
import math
import jax
import jax.numpy as jnp
from jax import lax

STATE = 137
PROF = 8
MEMBERS = 64
CHANNELS = 8704


def place_ends(result, own_key, low, top_value):
    place = [jax.random.randint(jax.random.fold_in(own_key, axis), (), 0, length) for axis, length in enumerate(result.shape)]
    longest = result.shape.index(max(result.shape))
    neighbour = place[:longest] + [(place[longest] + 1) % result.shape[longest]] + place[longest + 1:]
    return result.at[tuple(place)].set(low).at[tuple(neighbour)].set(top_value)


def levels(stream_key, dims, pieces, least, top_value):
    loudness, own = 1.0, jax.random.fold_in(stream_key, 6)
    for position, shards_of in pieces:
        heights = jnp.exp(jax.random.uniform(jax.random.fold_in(own, position), (shards_of,), jnp.float32, least / len(pieces), top_value / len(pieces)))
        loudness = loudness * jnp.repeat(heights, dims[position] // shards_of).reshape([-1 if axis == position else 1 for axis in range(len(dims))])
    return loudness


def bell_draw(rng, dims, deviation, reach, pieces=(), held_as=jnp.bfloat16):
    array = jax.random.normal(rng, dims, jnp.float32) * deviation
    if len(pieces) > 0:
        array = levels(rng, dims, pieces, -0.22, 0.18) * array
    return jnp.clip(array, min=-reach, max=reach).astype(held_as)


def setup_inputs(seed: int = 0) -> dict:
    keys = jax.random.split(jax.random.key(seed), 6)
    return {
        "state_anom": bell_draw(keys[0], (PROF, MEMBERS, STATE), 1.0, 6.0, ((1, 8),)),
        "radiance_anom": bell_draw(keys[1], (PROF, MEMBERS, CHANNELS), 1.0, 6.0, ((1, 8), (2, 4))),
        "inv_noise": jnp.clip(jnp.exp(math.log(0.2) - 2.3025851 * jax.random.uniform(keys[2], (CHANNELS,), jnp.float32) ** levels(keys[2], (CHANNELS,), ((0, 4),), -0.2, 0.2)), 0.02, 0.2),
        "innovation": bell_draw(keys[3], (PROF, CHANNELS), 1.0, 6.0, ((1, 4),), jnp.float32),
        "valid_count": place_ends(jax.random.randint(keys[4], (PROF,), CHANNELS // 2, min(CHANNELS, 8461) + 1), jax.random.fold_in(keys[4], 1), CHANNELS // 2, min(CHANNELS, 8461)).astype(jnp.int32),
    }


def reference(state_anom, radiance_anom, inv_noise, innovation, valid_count):
    cross = jnp.einsum('pmc,pms->pcs', radiance_anom.astype(jnp.float32), state_anom.astype(jnp.float32), precision=lax.Precision.HIGHEST)
    cross = cross / jnp.float32(MEMBERS - 1)
    slots = jnp.arange(CHANNELS, dtype=jnp.int32)
    valid = (slots[None, :] < valid_count[:, None].astype(jnp.int32)).astype(jnp.float32)
    weight = inv_noise[None, :] * valid
    weighted = cross * weight[:, :, None]
    information = jnp.einsum('pcs,pct->pst', weighted, cross, precision=lax.Precision.HIGHEST)
    gradient = jnp.einsum('pcs,pc->ps', weighted, innovation, precision=lax.Precision.HIGHEST)
    system = information + jnp.eye(STATE, dtype=jnp.float32)[None]
    increment = jnp.linalg.solve(system, gradient[:, :, None])[:, :, 0]
    return (information, gradient, increment)
```

```python
import functools
import jax
import jax.numpy as jnp
from jax import lax
from jax.experimental import pallas as pl
from jax.experimental.pallas import tpu as pltpu
from jax.sharding import PartitionSpec as P

F32, BF16 = jnp.float32, jnp.bfloat16
LANES, SUB = 128, 8
PARTS = 4
STEP = 16
ROUNDING = 2.0 ** -20
MIB = 1024 * 1024


def up(x, to):
    return -(-x // to) * to


def split3(x):
    a = x.astype(BF16)
    rest = x - a.astype(F32)
    b = rest.astype(BF16)
    c = (rest - b.astype(F32)).astype(BF16)
    return a, b, c


def pieces(width, count):
    tiles = width // LANES
    marks = [(tiles - tiles * i // count) * LANES for i in range(count, 0, -1)] + [width]
    return list(zip(marks[:-1], marks[1:]))


def partner(me, k, n):
    if n & (n - 1):
        return lax.rem(me + k, n)
    other, bit = me, 1
    while bit < n:
        if k & bit:
            other = other + bit * (1 - 2 * lax.rem(me // bit, 2))
        bit *= 2
    return other


def cholesky_rows(square, total):
    lanes = square.shape[1]
    rid8 = lax.broadcasted_iota(jnp.int32, (SUB, lanes), 0)
    cid = lax.broadcasted_iota(jnp.int32, square.shape, 1)
    rid = lax.broadcasted_iota(jnp.int32, square.shape, 0)
    least = jnp.sum(jnp.where(cid == rid, square, 0.0), axis=1, keepdims=True) * ROUNDING
    least = jnp.broadcast_to(least, square.shape)
    live, upper = square, []
    for p in range(0, total, SUB):
        steps = min(SUB, total - p)
        cols = [jnp.broadcast_to(live[:, p + j:p + j + 1], live.shape) for j in range(steps)]
        block, below = live[:SUB], live[SUB:]
        rows = jnp.zeros((SUB, lanes), F32)
        for j in range(steps):
            pivot = cols[j][j:j + 1]
            inverse = jnp.where(pivot > least[p + j:p + j + 1], lax.rsqrt(pivot), 0.0)
            column = cols[j] * inverse
            row = block[j:j + 1] * inverse
            rows = jnp.where(rid8 == j, jnp.broadcast_to(row, rows.shape), rows)
            for later in range(j + 1, steps):
                cols[later] = cols[later] - column * (cols[later][j:j + 1] * inverse)
            block = block - column[:SUB] * row
            if p + SUB < total:
                below = below - column[SUB:] * row
        lane = lax.broadcasted_iota(jnp.int32, (SUB, lanes), 1)
        upper.append(jnp.where(lane >= rid8 + p, rows, 0.0))
        live = below
    return jnp.concatenate(upper, 0)


def gram_kernel(n_mem, n_chan, parts_of_slab, count_hbm, state_hbm, rad_hbm, noise_hbm, innov_hbm,
                gram_ref, states_ref, *rest):
    factor_refs = rest[:-12]
    (count, mine, mine_states, noise, innov, held, held_states, parts,
     local_sem, mem_sem, small_sem, chan_sem) = rest[-12:]
    me, slab = lax.axis_index("mem"), lax.axis_index("chan")
    members, width = rad_hbm.shape[1:]
    states = state_hbm.shape[2]
    total = n_mem * members
    half = total // 2
    columns = parts.shape[2]

    barrier = pltpu.get_barrier_semaphore()
    for k in range(1, n_mem):
        pl.semaphore_signal(barrier, inc=1, device_id={"mem": partner(me, k, n_mem)})
    for k in range(1, n_chan):
        pl.semaphore_signal(barrier, inc=1, device_id={"chan": partner(slab, k, n_chan)})
    local = [
        pltpu.make_async_copy(src, dst, local_sem.at[i])
        for i, (src, dst) in enumerate((
            (state_hbm, mine_states), (rad_hbm, mine), (state_hbm.at[me], held_states.at[0]),
            (rad_hbm.at[me], held.at[0]), (count_hbm, count), (noise_hbm, noise), (innov_hbm, innov)))
    ]
    for copy in local:
        copy.start()
    for copy in local[:2]:
        copy.wait()
    pl.semaphore_wait(barrier, n_mem - 1 + n_chan - 1)

    small = []
    for k in range(n_mem - 1, 0, -1):
        peer = partner(me, k, n_mem)
        small.append(pltpu.make_async_remote_copy(
            src_ref=mine_states.at[peer], dst_ref=held_states.at[k],
            send_sem=small_sem.at[0, k], recv_sem=small_sem.at[1, k], device_id={"mem": peer}))
        small[-1].start()
    cuts = pieces(width, parts_of_slab)
    sends = []
    for c, (lo, hi) in enumerate(cuts):
        batch = []
        for k in range(n_mem - 1, 0, -1):
            peer = partner(me, k, n_mem)
            batch.append(pltpu.make_async_remote_copy(
                src_ref=mine.at[peer, :, lo:hi], dst_ref=held.at[k, :, lo:hi],
                send_sem=mem_sem.at[0, c, k], recv_sem=mem_sem.at[1, c, k], device_id={"mem": peer}))
            batch[-1].start()
        sends.append(batch)
    for copy in local[2:]:
        copy.wait()
    slots = slab * width + lax.broadcasted_iota(jnp.int32, (1, width), 1)
    weight = jnp.where(slots < count[me], noise[...].reshape(1, width), 0.0)
    pull = weight * innov[pl.ds(me, 1), :]
    pull = [part.astype(F32) for part in split3(pull)]

    for copy in small:
        copy.wait_recv()
    states_ref[...] = held_states[...]
    if factor_refs:
        anom = held_states[...].astype(F32).reshape(total, states)
        anom = jnp.concatenate([anom, jnp.zeros((total, up(states, LANES) - states), F32)], 1)
        tall = jnp.concatenate([anom, jnp.zeros((up(total, LANES) - total, anom.shape[1]), F32)], 0)
        square = lax.dot_general(anom.astype(BF16), tall.astype(BF16), (((1,), (1,)), ((), ())),
                                 preferred_element_type=F32)
        factor_refs[0][...] = cholesky_rows(square, total)
    extra = columns - total - half
    row = lax.broadcasted_iota(jnp.int32, (extra, 1), 0)
    acc = jnp.zeros((total, columns), F32)
    step = 2 * LANES
    for (start, stop), copies in zip(cuts, sends):
        for copy in copies:
            copy.wait_recv()
        for lo in range(start, stop, step):
            hi = min(lo + step, stop)
            block = held[:, :, lo:hi].astype(F32).reshape(total, hi - lo)
            scaled = block * weight[:, lo:hi]
            first = scaled.astype(BF16)
            second = (scaled - first.astype(F32)).astype(BF16)
            p0, p1, p2 = (part[:, lo:hi] for part in pull)
            even = lax.rem(row, 2) == 0
            tail0 = jnp.where(row < 4, jnp.where(even, p0, p2), 0.0).astype(BF16)
            tail1 = jnp.where((row < 4) & even, p1, 0.0).astype(BF16)
            block = block.astype(BF16)
            dims = (((1,), (1,)), ((), ()))
            acc += (
                lax.dot_general(block, jnp.concatenate([first, first[half:], tail0], 0), dims,
                                preferred_element_type=F32)
                + lax.dot_general(block, jnp.concatenate([second, second[half:], tail1], 0), dims,
                                  preferred_element_type=F32)
            )
    lane = lax.broadcasted_iota(jnp.int32, (half, columns), 1)
    upper = (lane < total) | ((lane >= total + half) & (lane < total + half + 2))
    parts[slab] = jnp.where(upper, acc[:half], acc[half:])

    shares = []
    for k in range(1, n_chan):
        shares.append(pltpu.make_async_remote_copy(
            src_ref=parts.at[slab], dst_ref=parts.at[slab],
            send_sem=chan_sem.at[0, k], recv_sem=chan_sem.at[1, k],
            device_id={"chan": partner(slab, k, n_chan)}))
        shares[-1].start()
    for copy in small + sum(sends, []):
        copy.wait_send()
    for copy in shares:
        copy.wait()
    whole = parts[0]
    for k in range(1, n_chan):
        whole = whole + parts[k]
    gram_ref[...] = whole


def eliminate(system, order):
    rows, lanes = system.shape
    rid = lax.broadcasted_iota(jnp.int32, (SUB, LANES), 0)

    def wide(piece, tiles):
        return piece if tiles == 1 else jnp.concatenate([piece] * tiles, 1)

    for p in range(0, order, STEP):
        steps = min(STEP, order - p)
        size = up(steps, SUB)
        base = p // LANES * LANES
        tiles = (lanes - base) // LANES
        live = system[:, base:]
        at = p - base
        block = [live[p + i:p + i + SUB] for i in range(0, size, SUB)]
        cols = [[jnp.broadcast_to(b[:, at + j:at + j + 1], (SUB, LANES)) for b in block] for j in range(steps)]
        far = jnp.concatenate(([live[:p]] if p else []) + ([live[p + size:]] if p + size < rows else []), 0) \
            if size < rows else None
        for j in range(steps):
            home, k = divmod(j, SUB)
            inverse = 1.0 / cols[j][home][k:k + 1, :]
            pivot_row = block[home][k:k + 1, :] * wide(inverse, tiles)
            for later in range(j + 1, steps):
                c = cols[later]
                scale = c[home][k:k + 1, :] * inverse
                new = [c[i] - cols[j][i] * scale for i in range(len(c))]
                new[home] = jnp.where(rid == k, jnp.broadcast_to(scale, (SUB, LANES)), new[home])
                cols[later] = new
            new = [b - wide(cols[j][i], tiles) * pivot_row for i, b in enumerate(block)]
            new[home] = jnp.where(wide(rid, tiles) == k, jnp.broadcast_to(pivot_row, new[home].shape), new[home])
            block = new
        if far is not None:
            for j in range(steps):
                home, k = divmod(j, SUB)
                scale = jnp.broadcast_to(live_column(live, p, size, at + j), (rows - size, LANES))
                far = far - wide(scale, tiles) * block[home][k:k + 1, :]
        out = ([far[:p]] if p else []) + block + ([far[p:]] if p + size < rows else [])
        live = jnp.concatenate(out, 0) if len(out) > 1 else out[0]
        system = live if base == 0 else jnp.concatenate([system[:, :base], live], 1)
    return system[:, order:order + 1]


def live_column(live, p, size, at):
    rows = live.shape[0]
    column = ([live[:p, at:at + 1]] if p else []) + ([live[p + size:, at:at + 1]] if p + size < rows else [])
    return jnp.concatenate(column, 0) if len(column) > 1 else column[0]


def unfold(packed, total):
    half = total // 2
    top, last = packed[:, :total], packed[:, total:total + half]
    low = jnp.concatenate([top[:, half:].T, last], 1)
    first = total + half
    force = jnp.concatenate([packed[:, i:i + 1] + packed[:, i + 1:i + 2] for i in (first, first + 2)], 0)
    return jnp.concatenate([top, low], 0), force


def solve_kernel(total, gram_ref, states_ref, *rest):
    factor_refs, (info_ref, grad_ref, inc_ref) = rest[:-3], rest[-3:]
    states = states_ref.shape[2]
    scale = 1.0 / (total - 1)
    rows, lanes = up(states, SUB), up(states + 1, LANES)
    depth = up(total + 1, LANES)
    anom = states_ref[...].astype(F32).reshape(total, states)
    anom = jnp.concatenate([anom, jnp.zeros((total, lanes - states), F32)], 1)
    square, force = unfold(gram_ref[...], total)
    gram = jnp.concatenate([square, force, jnp.zeros((total, depth - total - 1), F32)], 1)
    gradient = jnp.sum((force * scale) * anom, axis=0, keepdims=True)
    grad_ref[...] = gradient[:, :states]
    deep = jnp.concatenate([anom, jnp.zeros((depth - total, lanes), F32)], 0).astype(BF16)
    if factor_refs:
        factor = factor_refs[0][...]
        mixed = jnp.dot(factor[:, :total], gram, precision=lax.Precision.HIGHEST, preferred_element_type=F32)
        full = jnp.concatenate([factor, jnp.zeros((depth - total, factor.shape[1]), F32)], 0)
        system = lax.dot_general(mixed, full, (((1,), (1,)), ((), ())), precision=lax.Precision.HIGHEST,
                                 preferred_element_type=F32) * (scale * scale)
        rid = lax.broadcasted_iota(jnp.int32, system.shape, 0)
        cid = lax.broadcasted_iota(jnp.int32, system.shape, 1)
        system = system + jnp.where(rid == cid, 1.0, 0.0)
        system = jnp.where(cid == total, mixed, system)
        moved = functools.reduce(
            lambda a, b: b + a,
            [jnp.dot(m, deep, preferred_element_type=F32) for m in split3(mixed)][::-1]) * (scale * scale * scale)
        step = eliminate(system, total)
        inc_ref[...] = (gradient - jnp.sum(step * moved, axis=0, keepdims=True))[:, :states]
    turned = anom.T[:rows].astype(BF16)
    half = functools.reduce(
        lambda a, b: b + a,
        [jnp.dot(turned, g, preferred_element_type=F32) for g in split3(gram)][::-1])
    grad = half[:, total:total + 1] * scale
    info = functools.reduce(
        lambda a, b: b + a,
        [jnp.dot(h, deep, preferred_element_type=F32) for h in split3(half)][::-1])
    info = info * (scale * scale)
    info_ref[:, 0, :] = info[:states, :states]
    if factor_refs:
        return
    rid = lax.broadcasted_iota(jnp.int32, (rows, lanes), 0)
    cid = lax.broadcasted_iota(jnp.int32, (rows, lanes), 1)
    system = info + jnp.where(rid == cid, 1.0, 0.0)
    system = jnp.where(cid == states, jnp.broadcast_to(grad, (rows, lanes)), system)
    step = eliminate(system, states)
    lid = lax.broadcasted_iota(jnp.int32, (rows, LANES), 1)
    pair = jnp.where(lid == 1, step, 0.0)
    pair = jnp.concatenate([pair, jnp.zeros((lanes - rows, LANES), F32)], 0).T
    inc_ref[...] = pair[1:2, :states]


def shards(state_anom, radiance_anom, inv_noise, innovation, valid_count):
    n_mem, n_chan = lax.axis_size("mem"), lax.axis_size("chan")
    members, states = state_anom.shape[1:]
    width = radiance_anom.shape[2]
    total = members * n_mem
    half = total // 2
    columns = up(total + half + 16, LANES)
    vmem, far = pl.BlockSpec(memory_space=pltpu.VMEM), pl.BlockSpec(memory_space=pltpu.HBM)
    dma = pltpu.SemaphoreType.DMA
    factor = () if total > states else (jax.ShapeDtypeStruct((total, up(total, LANES)), F32),)
    valid_count, state_anom, radiance_anom, inv_noise, innovation = (pltpu.with_memory_space_constraint(x, pltpu.HBM) for x in (valid_count, state_anom, radiance_anom, inv_noise, innovation))
    gram, own_states, *factors = pl.pallas_call(
        functools.partial(gram_kernel, n_mem, n_chan, PARTS),
        out_shape=(jax.ShapeDtypeStruct((half, columns), F32),
                   jax.ShapeDtypeStruct((n_mem, members, states), BF16)) + factor,
        in_specs=[far] * 5,
        out_specs=(vmem,) * (2 + len(factor)),
        scratch_shapes=[
            pltpu.SMEM(valid_count.shape, jnp.int32),
            pltpu.VMEM((n_mem, members, width), BF16),
            pltpu.VMEM((n_mem, members, states), BF16),
            pltpu.VMEM((width,), F32),
            pltpu.VMEM(innovation.shape, F32),
            pltpu.VMEM((n_mem, members, width), BF16),
            pltpu.VMEM((n_mem, members, states), BF16),
            pltpu.VMEM((n_chan, half, columns), F32),
            dma((7,)), dma((2, PARTS, n_mem)), dma((2, n_mem)), dma((2, n_chan)),
        ],
        compiler_params=pltpu.CompilerParams(
            collective_id=0, has_side_effects=True, vmem_limit_bytes=24 * MIB),
    )(valid_count, state_anom, radiance_anom, inv_noise, innovation)
    information, gradient, increment = pl.pallas_call(
        functools.partial(solve_kernel, total),
        out_shape=(jax.ShapeDtypeStruct((states, 1, states), F32),
                   jax.ShapeDtypeStruct((1, states), F32),
                   jax.ShapeDtypeStruct((1, states), F32)),
        in_specs=[vmem] * (2 + len(factor)),
        out_specs=(vmem, vmem, vmem),
        compiler_params=pltpu.CompilerParams(vmem_limit_bytes=24 * MIB),
    )(gram, own_states, *factors)
    return information.transpose(1, 0, 2), gradient, increment


def solution(mesh):
    in_specs = (P(None, "mem", None), P(None, "mem", "chan"), P("chan"), P(None, "chan"), P())
    out_specs = (P("mem", None, None), P("mem", None), P("mem", None))
    return jax.shard_map(shards, mesh=mesh, in_specs=in_specs, out_specs=out_specs, check_vma=False)
```

```python
import functools
import jax
import jax.numpy as jnp
from jax import lax
from jax.experimental import pallas as pl
from jax.experimental.pallas import tpu as pltpu
from jax.sharding import PartitionSpec as P

F32, BF16 = jnp.float32, jnp.bfloat16
LANES, SUB = 128, 8
PARTS = 3
STEP = 16
ROUNDING = 2.0 ** -20
MIB = 1024 * 1024


def up(x, to):
    return -(-x // to) * to


def split3(x):
    a = x.astype(BF16)
    rest = x - a.astype(F32)
    b = rest.astype(BF16)
    c = (rest - b.astype(F32)).astype(BF16)
    return a, b, c


def pieces(width, count):
    tiles = width // LANES
    marks = [(tiles - tiles * i // count) * LANES for i in range(count, 0, -1)] + [width]
    return list(zip(marks[:-1], marks[1:]))


def partner(me, k, n):
    if n & (n - 1):
        return lax.rem(me + k, n)
    other, bit = me, 1
    while bit < n:
        other = other + (k // bit % 2) * bit * (1 - 2 * (me // bit % 2))
        bit *= 2
    return other


def cholesky_rows(square, total):
    lanes = square.shape[1]
    rid8 = lax.broadcasted_iota(jnp.int32, (SUB, lanes), 0)
    cid = lax.broadcasted_iota(jnp.int32, square.shape, 1)
    rid = lax.broadcasted_iota(jnp.int32, square.shape, 0)
    least = jnp.sum(jnp.where(cid == rid, square, 0.0), axis=1, keepdims=True) * ROUNDING
    least = jnp.broadcast_to(least, square.shape)
    live, upper = square, []
    for p in range(0, total, SUB):
        steps = min(SUB, total - p)
        cols = [jnp.broadcast_to(live[:, p + j:p + j + 1], live.shape) for j in range(steps)]
        block, below = live[:SUB], live[SUB:]
        rows = jnp.zeros((SUB, lanes), F32)
        for j in range(steps):
            pivot = cols[j][j:j + 1]
            inverse = jnp.where(pivot > least[p + j:p + j + 1], lax.rsqrt(pivot), 0.0)
            column = cols[j] * inverse
            row = block[j:j + 1] * inverse
            rows = jnp.where(rid8 == j, jnp.broadcast_to(row, rows.shape), rows)
            for later in range(j + 1, steps):
                cols[later] = cols[later] - column * (cols[later][j:j + 1] * inverse)
            block = block - column[:SUB] * row
            if p + SUB < total:
                below = below - column[SUB:] * row
        lane = lax.broadcasted_iota(jnp.int32, (SUB, lanes), 1)
        upper.append(jnp.where(lane >= rid8 + p, rows, 0.0))
        live = below
    return jnp.concatenate(upper, 0)


def gram_kernel(n_mem, n_chan, parts_of_slab, count_hbm, state_hbm, rad_hbm, noise_hbm, innov_hbm,
                gram_ref, states_ref, *rest):
    factor_refs = rest[:-14]
    (count, mine, mine_states, noise, innov, held, held_states, parts,
     local_sem, mem_sem, near_sem, far_sem, relay_sem, chan_sem) = rest[-14:]
    me, slab = lax.axis_index("mem"), lax.axis_index("chan")
    members, width = rad_hbm.shape[1:]
    states = state_hbm.shape[2]
    total = n_mem * members
    half = total // 2
    columns = parts.shape[2]

    barrier = pltpu.get_barrier_semaphore()
    for k in range(1, n_mem):
        pl.semaphore_signal(barrier, inc=1, device_id={"mem": partner(me, k, n_mem)})
    for k in range(1, n_chan):
        pl.semaphore_signal(barrier, inc=1, device_id={"chan": partner(slab, k, n_chan)})
    local = [
        pltpu.make_async_copy(src, dst, local_sem.at[i])
        for i, (src, dst) in enumerate((
            (state_hbm, mine_states), (rad_hbm, mine), (count_hbm, count), (noise_hbm, noise), (innov_hbm, innov)))
    ]
    for copy in local:
        copy.start()
    for copy in local[:2]:
        copy.wait()
    pl.semaphore_wait(barrier, n_mem - 1 + n_chan - 1)

    near = n_mem // 2
    shared = near // n_chan if n_mem & (n_mem - 1) == 0 and near % n_chan == 0 else 0
    direct = near if shared else n_mem

    def state_copy(k, sems):
        peer = partner(me, k, n_mem)
        return pltpu.make_async_remote_copy(
            src_ref=mine_states.at[peer], dst_ref=held_states.at[k],
            send_sem=sems.at[0], recv_sem=sems.at[1], device_id={"mem": peer})

    def blocks(source, target, sems):
        return pltpu.make_async_remote_copy(
            src_ref=source, dst_ref=target, send_sem=sems.at[0], recv_sem=sems.at[1],
            device_id={"mem": partner(me, 1, n_mem)})

    far = [state_copy(near + i * n_chan + slab, far_sem.at[i]) for i in range(shared)]
    for copy in far:
        copy.start()
    for k in range(direct - 1, 0, -1):
        state_copy(k, near_sem).start()
    all_states = blocks(mine_states.at[1:direct], held_states.at[1:direct], near_sem)
    cuts = pieces(width, parts_of_slab)
    sends = []
    for c, (lo, hi) in enumerate(cuts):
        for k in range(n_mem - 1, 0, -1):
            peer = partner(me, k, n_mem)
            pltpu.make_async_remote_copy(
                src_ref=mine.at[peer, :, lo:hi], dst_ref=held.at[k, :, lo:hi],
                send_sem=mem_sem.at[c, 0], recv_sem=mem_sem.at[c, 1], device_id={"mem": peer}).start()
        sends.append(blocks(mine.at[1:, :, lo:hi], held.at[1:, :, lo:hi], mem_sem.at[c]))
    for copy in local[2:]:
        copy.wait()
    slots = slab * width + lax.broadcasted_iota(jnp.int32, (1, width), 1)
    weight = jnp.where(slots < count[me], noise[...].reshape(1, width), 0.0)
    pull = weight * innov[pl.ds(me, 1), :]
    pull = [part.astype(F32) for part in split3(pull)]

    relays = []
    for i, copy in enumerate(far):
        copy.wait_recv()
        k = near + i * n_chan + slab
        for j in range(1, n_chan):
            pltpu.make_async_remote_copy(
                src_ref=held_states.at[k], dst_ref=held_states.at[k], send_sem=relay_sem.at[0],
                recv_sem=relay_sem.at[1], device_id={"chan": partner(slab, j, n_chan)}).start()
    if shared:
        size = shared * (n_chan - 1)
        relays.append(blocks(mine_states.at[:size], held_states.at[:size], relay_sem))
    def whole(own, others, lo, hi):
        parts_of = [own[pl.ds(me, 1), :, lo:hi], others[1:, :, lo:hi]]
        return jnp.concatenate([part.astype(F32).reshape(-1, hi - lo) for part in parts_of], 0)

    extra = columns - total - half
    row = lax.broadcasted_iota(jnp.int32, (extra, 1), 0)
    acc = jnp.zeros((total, columns), F32)
    step = 2 * LANES
    for (start, stop), copy in zip(cuts, sends):
        copy.wait_recv()
        for lo in range(start, stop, step):
            hi = min(lo + step, stop)
            block = whole(mine, held, lo, hi)
            scaled = block * weight[:, lo:hi]
            first = scaled.astype(BF16)
            second = (scaled - first.astype(F32)).astype(BF16)
            p0, p1, p2 = (part[:, lo:hi] for part in pull)
            even = lax.rem(row, 2) == 0
            tail0 = jnp.where(row < 4, jnp.where(even, p0, p2), 0.0).astype(BF16)
            tail1 = jnp.where((row < 4) & even, p1, 0.0).astype(BF16)
            block = block.astype(BF16)
            dims = (((1,), (1,)), ((), ()))
            acc += (
                lax.dot_general(block, jnp.concatenate([first, first[half:], tail0], 0), dims,
                                preferred_element_type=F32)
                + lax.dot_general(block, jnp.concatenate([second, second[half:], tail1], 0), dims,
                                  preferred_element_type=F32)
            )
    lane = lax.broadcasted_iota(jnp.int32, (half, columns), 1)
    upper = (lane < total) | ((lane >= total + half) & (lane < total + half + 2))
    parts[slab] = jnp.where(upper, acc[:half], acc[half:])

    for k in range(1, n_chan):
        pltpu.make_async_remote_copy(
            src_ref=parts.at[slab], dst_ref=parts.at[slab], send_sem=chan_sem.at[0], recv_sem=chan_sem.at[1],
            device_id={"chan": partner(slab, k, n_chan)}).start()
    all_states.wait_recv()
    for copy in relays:
        copy.wait_recv()
    states_ref[pl.ds(0, 1)] = mine_states[pl.ds(me, 1)]
    states_ref[1:] = held_states[1:]
    if factor_refs:
        anom = whole(mine_states, held_states, 0, states)
        anom = jnp.concatenate([anom, jnp.zeros((total, up(states, LANES) - states), F32)], 1)
        tall = jnp.concatenate([anom, jnp.zeros((up(total, LANES) - total, anom.shape[1]), F32)], 0)
        square = lax.dot_general(anom.astype(BF16), tall.astype(BF16), (((1,), (1,)), ((), ())),
                                 preferred_element_type=F32)
        factor_refs[0][...] = cholesky_rows(square, total)
    for copy in [all_states] + far + sends + relays:
        copy.wait_send()
    blocks(parts.at[:n_chan - 1], parts.at[:n_chan - 1], chan_sem).wait()
    summed = parts[0]
    for k in range(1, n_chan):
        summed = summed + parts[k]
    gram_ref[...] = summed


def eliminate(system, order):
    rows, lanes = system.shape
    rid = lax.broadcasted_iota(jnp.int32, (SUB, LANES), 0)

    def wide(piece, tiles):
        return piece if tiles == 1 else jnp.concatenate([piece] * tiles, 1)

    for p in range(0, order, STEP):
        steps = min(STEP, order - p)
        size = up(steps, SUB)
        base = p // LANES * LANES
        tiles = (lanes - base) // LANES
        live = system[:, base:]
        at = p - base
        block = [live[p + i:p + i + SUB] for i in range(0, size, SUB)]
        cols = [[jnp.broadcast_to(b[:, at + j:at + j + 1], (SUB, LANES)) for b in block] for j in range(steps)]
        far = jnp.concatenate(([live[:p]] if p else []) + ([live[p + size:]] if p + size < rows else []), 0) \
            if size < rows else None
        for j in range(steps):
            home, k = divmod(j, SUB)
            inverse = 1.0 / cols[j][home][k:k + 1, :]
            pivot_row = block[home][k:k + 1, :] * wide(inverse, tiles)
            for later in range(j + 1, steps):
                c = cols[later]
                scale = c[home][k:k + 1, :] * inverse
                new = [c[i] - cols[j][i] * scale for i in range(len(c))]
                new[home] = jnp.where(rid == k, jnp.broadcast_to(scale, (SUB, LANES)), new[home])
                cols[later] = new
            new = [b - wide(cols[j][i], tiles) * pivot_row for i, b in enumerate(block)]
            new[home] = jnp.where(wide(rid, tiles) == k, jnp.broadcast_to(pivot_row, new[home].shape), new[home])
            block = new
        if far is not None:
            for j in range(steps):
                home, k = divmod(j, SUB)
                scale = jnp.broadcast_to(live_column(live, p, size, at + j), (rows - size, LANES))
                far = far - wide(scale, tiles) * block[home][k:k + 1, :]
        out = ([far[:p]] if p else []) + block + ([far[p:]] if p + size < rows else [])
        live = jnp.concatenate(out, 0) if len(out) > 1 else out[0]
        system = live if base == 0 else jnp.concatenate([system[:, :base], live], 1)
    return system[:, order:order + 1]


def live_column(live, p, size, at):
    rows = live.shape[0]
    column = ([live[:p, at:at + 1]] if p else []) + ([live[p + size:, at:at + 1]] if p + size < rows else [])
    return jnp.concatenate(column, 0) if len(column) > 1 else column[0]


def unfold(packed, total):
    half = total // 2
    top, last = packed[:, :total], packed[:, total:total + half]
    low = jnp.concatenate([top[:, half:].T, last], 1)
    first = total + half
    force = jnp.concatenate([packed[:, i:i + 1] + packed[:, i + 1:i + 2] for i in (first, first + 2)], 0)
    return jnp.concatenate([top, low], 0), force


def solve_kernel(total, gram_ref, states_ref, *rest):
    factor_refs, (info_ref, grad_ref, inc_ref) = rest[:-3], rest[-3:]
    states = states_ref.shape[2]
    scale = 1.0 / (total - 1)
    rows, lanes = up(states, SUB), up(states + 1, LANES)
    depth = up(total + 1, LANES)
    anom = states_ref[...].astype(F32).reshape(total, states)
    anom = jnp.concatenate([anom, jnp.zeros((total, lanes - states), F32)], 1)
    square, force = unfold(gram_ref[...], total)
    gram = jnp.concatenate([square, force, jnp.zeros((total, depth - total - 1), F32)], 1)
    gradient = jnp.sum((force * scale) * anom, axis=0, keepdims=True)
    grad_ref[...] = gradient[:, :states]
    deep = jnp.concatenate([anom, jnp.zeros((depth - total, lanes), F32)], 0).astype(BF16)
    if factor_refs:
        factor = factor_refs[0][...]
        mixed = jnp.dot(factor[:, :total], gram, precision=lax.Precision.HIGHEST, preferred_element_type=F32)
        full = jnp.concatenate([factor, jnp.zeros((depth - total, factor.shape[1]), F32)], 0)
        system = lax.dot_general(mixed, full, (((1,), (1,)), ((), ())), precision=lax.Precision.HIGHEST,
                                 preferred_element_type=F32) * (scale * scale)
        rid = lax.broadcasted_iota(jnp.int32, system.shape, 0)
        cid = lax.broadcasted_iota(jnp.int32, system.shape, 1)
        system = system + jnp.where(rid == cid, 1.0, 0.0)
        system = jnp.where(cid == total, mixed, system)
        moved = functools.reduce(
            lambda a, b: b + a,
            [jnp.dot(m, deep, preferred_element_type=F32) for m in split3(mixed)][::-1]) * (scale * scale * scale)
        step = eliminate(system, total)
        inc_ref[...] = (gradient - jnp.sum(step * moved, axis=0, keepdims=True))[:, :states]
    turned = anom.T[:rows].astype(BF16)
    half = functools.reduce(
        lambda a, b: b + a,
        [jnp.dot(turned, g, preferred_element_type=F32) for g in split3(gram)][::-1])
    grad = half[:, total:total + 1] * scale
    info = functools.reduce(
        lambda a, b: b + a,
        [jnp.dot(h, deep, preferred_element_type=F32) for h in split3(half)][::-1])
    info = info * (scale * scale)
    info_ref[:, 0, :] = info[:states, :states]
    if factor_refs:
        return
    rid = lax.broadcasted_iota(jnp.int32, (rows, lanes), 0)
    cid = lax.broadcasted_iota(jnp.int32, (rows, lanes), 1)
    system = info + jnp.where(rid == cid, 1.0, 0.0)
    system = jnp.where(cid == states, jnp.broadcast_to(grad, (rows, lanes)), system)
    step = eliminate(system, states)
    lid = lax.broadcasted_iota(jnp.int32, (rows, LANES), 1)
    pair = jnp.where(lid == 1, step, 0.0)
    pair = jnp.concatenate([pair, jnp.zeros((lanes - rows, LANES), F32)], 0).T
    inc_ref[...] = pair[1:2, :states]


def shards(state_anom, radiance_anom, inv_noise, innovation, valid_count):
    n_mem, n_chan = lax.axis_size("mem"), lax.axis_size("chan")
    members, states = state_anom.shape[1:]
    width = radiance_anom.shape[2]
    total = members * n_mem
    half = total // 2
    columns = up(total + half + 16, LANES)
    vmem, far = pl.BlockSpec(memory_space=pltpu.VMEM), pl.BlockSpec(memory_space=pltpu.HBM)
    dma = pltpu.SemaphoreType.DMA
    factor = () if total > states else (jax.ShapeDtypeStruct((total, up(total, LANES)), F32),)
    valid_count, state_anom, radiance_anom, inv_noise, innovation = (pltpu.with_memory_space_constraint(x, pltpu.HBM) for x in (valid_count, state_anom, radiance_anom, inv_noise, innovation))
    gram, own_states, *factors = pl.pallas_call(
        functools.partial(gram_kernel, n_mem, n_chan, PARTS),
        out_shape=(jax.ShapeDtypeStruct((half, columns), F32),
                   jax.ShapeDtypeStruct((n_mem, members, states), BF16)) + factor,
        in_specs=[far] * 5,
        out_specs=(vmem,) * (2 + len(factor)),
        scratch_shapes=[
            pltpu.SMEM(valid_count.shape, jnp.int32),
            pltpu.VMEM((n_mem, members, width), BF16),
            pltpu.VMEM((n_mem, members, states), BF16),
            pltpu.VMEM((width,), F32),
            pltpu.VMEM(innovation.shape, F32),
            pltpu.VMEM((n_mem, members, width), BF16),
            pltpu.VMEM((n_mem, members, states), BF16),
            pltpu.VMEM((n_chan, half, columns), F32),
            dma((5,)), dma((PARTS, 2)), dma((2,)), dma((max(n_mem // 2 // n_chan, 1), 2)), dma((2,)), dma((2,)),
        ],
        compiler_params=pltpu.CompilerParams(
            collective_id=0, has_side_effects=True, vmem_limit_bytes=24 * MIB),
    )(valid_count, state_anom, radiance_anom, inv_noise, innovation)
    information, gradient, increment = pl.pallas_call(
        functools.partial(solve_kernel, total),
        out_shape=(jax.ShapeDtypeStruct((states, 1, states), F32),
                   jax.ShapeDtypeStruct((1, states), F32),
                   jax.ShapeDtypeStruct((1, states), F32)),
        in_specs=[vmem] * (2 + len(factor)),
        out_specs=(vmem, vmem, vmem),
        compiler_params=pltpu.CompilerParams(vmem_limit_bytes=24 * MIB),
    )(gram, own_states, *factors)
    return information.transpose(1, 0, 2), gradient, increment


def solution(mesh):
    in_specs = (P(None, "mem", None), P(None, "mem", "chan"), P("chan"), P(None, "chan"), P())
    out_specs = (P("mem", None, None), P("mem", None), P("mem", None))
    return jax.shard_map(shards, mesh=mesh, in_specs=in_specs, out_specs=out_specs, check_vma=False)
```

```python
import functools
import jax
import jax.numpy as jnp
from jax import lax
from jax.experimental import pallas as pl
from jax.experimental.pallas import tpu as pltpu
from jax.sharding import PartitionSpec as P

F32, BF16 = jnp.float32, jnp.bfloat16
LANES, SUB = 128, 8
PARTS = 1
STEP = 16
ROUNDING = 2.0 ** -20
MIB = 1024 * 1024


def up(x, to):
    return -(-x // to) * to


def split2(x):
    a = x.astype(BF16)
    return a, (x - a.astype(F32)).astype(BF16)


def split3(x):
    a = x.astype(BF16)
    return (a,) + split2(x - a.astype(F32))


def pieces(width, count):
    tiles = width // LANES
    marks = [(tiles - tiles * i // count) * LANES for i in range(count, 0, -1)] + [width]
    return list(zip(marks[:-1], marks[1:]))


def partner(me, k, n):
    if n & (n - 1):
        return lax.rem(me + k, n)
    other, bit = me, 1
    while bit < n:
        other = other + (k // bit % 2) * bit * (1 - 2 * (me // bit % 2))
        bit *= 2
    return other


def cholesky_rows(square, total):
    lanes = square.shape[1]
    rid8 = lax.broadcasted_iota(jnp.int32, (SUB, lanes), 0)
    cid = lax.broadcasted_iota(jnp.int32, square.shape, 1)
    rid = lax.broadcasted_iota(jnp.int32, square.shape, 0)
    least = jnp.sum(jnp.where(cid == rid, square, 0.0), axis=1, keepdims=True) * ROUNDING
    least = jnp.broadcast_to(least, square.shape)
    live, upper = square, []
    for p in range(0, total, SUB):
        steps = min(SUB, total - p)
        cols = [jnp.broadcast_to(live[:, p + j:p + j + 1], live.shape) for j in range(steps)]
        block, below = live[:SUB], live[SUB:]
        rows = jnp.zeros((SUB, lanes), F32)
        for j in range(steps):
            pivot = cols[j][j:j + 1]
            inverse = jnp.where(pivot > least[p + j:p + j + 1], lax.rsqrt(pivot), 0.0)
            column = cols[j] * inverse
            row = block[j:j + 1] * inverse
            rows = jnp.where(rid8 == j, jnp.broadcast_to(row, rows.shape), rows)
            for later in range(j + 1, steps):
                cols[later] = cols[later] - column * (cols[later][j:j + 1] * inverse)
            block = block - column[:SUB] * row
            if p + SUB < total:
                below = below - column[SUB:] * row
        lane = lax.broadcasted_iota(jnp.int32, (SUB, lanes), 1)
        upper.append(jnp.where(lane >= rid8 + p, rows, 0.0))
        live = below
    return jnp.concatenate(upper, 0)


def gram_kernel(n_mem, n_chan, parts_of_slab, count_hbm, state_hbm, rad_hbm, noise_hbm, innov_hbm,
                gram_ref, states_ref, *rest):
    factor_refs = rest[:-14]
    (count, mine, mine_states, noise, innov, held, held_states, parts,
     local_sem, mem_sem, near_sem, far_sem, relay_sem, chan_sem) = rest[-14:]
    me, slab = lax.axis_index("mem"), lax.axis_index("chan")
    members, width = rad_hbm.shape[1:]
    states = state_hbm.shape[2]
    total = n_mem * members
    columns = parts.shape[2]
    height = parts.shape[1] - SUB
    sent = height + (1 if columns == LANES else SUB)

    barrier = pltpu.get_barrier_semaphore()
    for k in range(1, n_mem):
        pl.semaphore_signal(barrier, inc=1, device_id={"mem": partner(me, k, n_mem)})
    for k in range(1, n_chan):
        pl.semaphore_signal(barrier, inc=1, device_id={"chan": partner(slab, k, n_chan)})
    local = [
        pltpu.make_async_copy(src, dst, local_sem.at[i])
        for i, (src, dst) in enumerate((
            (state_hbm, mine_states), (rad_hbm, mine), (count_hbm, count), (noise_hbm, noise), (innov_hbm, innov)))
    ]
    for copy in local:
        copy.start()
    for copy in local[:2]:
        copy.wait()
    pl.semaphore_wait(barrier, n_mem - 1 + n_chan - 1)

    near = n_mem // 2
    shared = near // n_chan if n_mem & (n_mem - 1) == 0 and near % n_chan == 0 else 0
    direct = near if shared else n_mem

    def state_copy(k, sems):
        peer = partner(me, k, n_mem)
        return pltpu.make_async_remote_copy(
            src_ref=mine_states.at[peer], dst_ref=held_states.at[k],
            send_sem=sems.at[0], recv_sem=sems.at[1], device_id={"mem": peer})

    def blocks(source, target, sems):
        return pltpu.make_async_remote_copy(
            src_ref=source, dst_ref=target, send_sem=sems.at[0], recv_sem=sems.at[1],
            device_id={"mem": partner(me, 1, n_mem)})

    far = [state_copy(near + i * n_chan + slab, far_sem.at[i]) for i in range(shared)]
    for copy in far:
        copy.start()
    for k in range(direct - 1, 0, -1):
        state_copy(k, near_sem).start()
    all_states = blocks(mine_states.at[1:direct], held_states.at[1:direct], near_sem)
    cuts = pieces(width, parts_of_slab)
    rounds = sorted(range(1, n_mem), key=lambda k: (k < near, k // 2 % 2, -k))
    sends = []
    for c, (lo, hi) in enumerate(cuts):
        for k in rounds:
            peer = partner(me, k, n_mem)
            pltpu.make_async_remote_copy(
                src_ref=mine.at[peer, :, lo:hi], dst_ref=held.at[k, :, lo:hi],
                send_sem=mem_sem.at[c, 0], recv_sem=mem_sem.at[c, 1], device_id={"mem": peer}).start()
        sends.append(blocks(mine.at[1:, :, lo:hi], held.at[1:, :, lo:hi], mem_sem.at[c]))
    for copy in local[2:]:
        copy.wait()
    slots = slab * width + lax.broadcasted_iota(jnp.int32, (1, width), 1)
    weight = jnp.where(slots < count[me], noise[...].reshape(1, width), 0.0)
    pull = weight * innov[pl.ds(me, 1), :]
    pull = [part.astype(F32) for part in split2(pull)]

    relays = []
    for i, copy in enumerate(far):
        copy.wait_recv()
        k = near + i * n_chan + slab
        for j in range(1, n_chan):
            pltpu.make_async_remote_copy(
                src_ref=held_states.at[k], dst_ref=held_states.at[k], send_sem=relay_sem.at[0],
                recv_sem=relay_sem.at[1], device_id={"chan": partner(slab, j, n_chan)}).start()
    if shared:
        size = shared * (n_chan - 1)
        relays.append(blocks(mine_states.at[:size], held_states.at[:size], relay_sem))
    def whole(own, others, lo, hi):
        parts_of = [own[pl.ds(me, 1), :, lo:hi], others[1:, :, lo:hi]]
        return jnp.concatenate([part.astype(F32).reshape(-1, hi - lo) for part in parts_of], 0)

    row = lax.broadcasted_iota(jnp.int32, (2 * SUB, 1), 0)
    acc = jnp.zeros((2 * total + 2 * SUB, columns), F32)
    step = 2 * LANES
    for (start, stop), copy in zip(cuts, sends):
        copy.wait_recv()
        for lo in range(start, stop, step):
            hi = min(lo + step, stop)
            block = whole(mine, held, lo, hi)
            first, second = split2(block * weight[:, lo:hi])
            tail = jnp.where(row == 0, pull[0][:, lo:hi], jnp.where(row == 1, pull[1][:, lo:hi], 0.0)).astype(BF16)
            block = jnp.concatenate([block.astype(BF16)] * (columns // total), 0)
            acc += lax.dot_general(jnp.concatenate([first, second, tail], 0), block, (((1,), (1,)), ((), ())),
                                   preferred_element_type=F32)
    square = acc[:total] + acc[total:2 * total]
    if columns > total:
        lane = lax.broadcasted_iota(jnp.int32, (height, columns), 1)
        square = jnp.where(lane < total, square[:height], square[height:])
    parts[slab, :height] = square
    parts[slab, height:] = jnp.broadcast_to(acc[2 * total:2 * total + 1] + acc[2 * total + 1:2 * total + 2],
                                            (SUB, columns))
    for k in range(1, n_chan):
        pltpu.make_async_remote_copy(
            src_ref=parts.at[slab, :sent], dst_ref=parts.at[slab, :sent], send_sem=chan_sem.at[0], recv_sem=chan_sem.at[1],
            device_id={"chan": partner(slab, k, n_chan)}).start()
    all_states.wait_recv()
    for copy in relays:
        copy.wait_recv()
    states_ref[pl.ds(0, 1)] = mine_states[pl.ds(me, 1)]
    states_ref[1:] = held_states[1:]
    if factor_refs:
        anom = whole(mine_states, held_states, 0, states)
        anom = jnp.concatenate([anom, jnp.zeros((total, up(states, LANES) - states), F32)], 1)
        tall = jnp.concatenate([anom, jnp.zeros((up(total, LANES) - total, anom.shape[1]), F32)], 0)
        square = lax.dot_general(anom.astype(BF16), tall.astype(BF16), (((1,), (1,)), ((), ())),
                                 preferred_element_type=F32)
        factor = cholesky_rows(square, total)
        factor_refs[0][...] = factor + pltpu.roll(factor, total, 1)
    for copy in [all_states] + far + sends + relays:
        copy.wait_send()
    arrived = parts.at[:n_chan - 1, :sent]
    blocks(arrived, arrived, chan_sem).wait()
    for rows in (slice(0, height), slice(height, height + 1)):
        summed = parts[0, rows]
        for k in range(1, n_chan):
            summed = summed + parts[k, rows]
        gram_ref[rows] = summed


def eliminate(system, order, right):
    rows, lanes = system.shape
    rid = lax.broadcasted_iota(jnp.int32, (SUB, LANES), 0)

    def wide(piece, tiles):
        return piece if tiles == 1 else jnp.concatenate([piece] * tiles, 1)

    for p in range(0, order, STEP):
        steps = min(STEP, order - p)
        size = up(steps, SUB)
        base = p // LANES * LANES
        tiles = (lanes - base) // LANES
        live = system[:, base:]
        at = p - base

        def others(x):
            kept = ([x[:p]] if p else []) + ([x[p + size:]] if p + size < rows else [])
            return (jnp.concatenate(kept, 0) if len(kept) > 1 else kept[0]) if kept else None

        def joined(inner, outer):
            out = ([outer[:p]] if p else []) + inner + ([outer[p:]] if p + size < rows else [])
            return jnp.concatenate(out, 0) if len(out) > 1 else out[0]

        block = [live[p + i:p + i + SUB] for i in range(0, size, SUB)]
        cols = [[jnp.broadcast_to(b[:, at + j:at + j + 1], (SUB, LANES)) for b in block] for j in range(steps)]
        cols.append([right[p + i:p + i + SUB] for i in range(0, size, SUB)])
        far, far_right = others(live), others(right)
        if far is not None:
            factors = [jnp.broadcast_to(far[:, at + j:at + j + 1], far_right.shape) for j in range(steps)]
        scales = [jnp.ones((SUB, LANES), F32)] * len(block)
        for j in range(steps):
            home, k = divmod(j, SUB)
            inverse = 1.0 / cols[j][home][k:k + 1, :]
            scales[home] = jnp.where(rid == k, inverse, scales[home])
            factor = list(cols[j])
            factor[home] = jnp.where(rid == k, 0.0, factor[home])
            for later in range(j + 1, steps + 1):
                c = cols[later]
                scale = c[home][k:k + 1, :] * inverse
                cols[later] = [c[i] - factor[i] * scale for i in range(len(c))]
            pivot_row = block[home][k:k + 1, :] * wide(inverse, tiles)
            block = [b - wide(factor[i], tiles) * pivot_row for i, b in enumerate(block)]
        block = [b * wide(s, tiles) for b, s in zip(block, scales)]
        solved = [c * s for c, s in zip(cols[steps], scales)]
        if far is not None:
            for j in range(steps):
                home, k = divmod(j, SUB)
                far = far - wide(factors[j], tiles) * block[home][k:k + 1, :]
                far_right = far_right - factors[j] * solved[home][k:k + 1, :]
        live = joined(block, far)
        right = joined(solved, far_right)
        system = live if base == 0 else jnp.concatenate([system[:, :base], live], 1)
    return right


def across(x, lane):
    return jnp.broadcast_to(x[:, lane:lane + 1], (x.shape[0], LANES))


def dots(*pairs):
    return functools.reduce(lambda a, b: a + b, [jnp.dot(a, b, preferred_element_type=F32) for a, b in pairs])


def solve_in_states(total, gram_ref, states_ref, info_ref, grad_ref, inc_ref):
    states = states_ref.shape[2]
    scale = 1.0 / (total - 1)
    rows, lanes = up(states, SUB), up(states, LANES)
    anom = states_ref[...].astype(F32).reshape(total, states)
    anom = jnp.concatenate([anom, jnp.zeros((total, lanes - states), F32)], 1)
    gram, force = gram_ref[:total], gram_ref[total:total + 1]
    gradient = jnp.dot(force, anom, precision=lax.Precision.HIGHEST, preferred_element_type=F32) * scale
    grad_ref[...] = gradient[:, :states]
    deep = anom.astype(BF16)
    turned = anom.T[:rows].astype(BF16)
    mixed = dots(*((turned, g) for g in split3(gram)[::-1]))
    info = dots(*((m, deep) for m in split3(mixed)[::-1])) * (scale * scale)
    info_ref[:, 0, :] = info[:states, :states]
    rid = lax.broadcasted_iota(jnp.int32, (rows, lanes), 0)
    cid = lax.broadcasted_iota(jnp.int32, (rows, lanes), 1)
    right = across(jnp.broadcast_to(gradient, (SUB, lanes)).T[:rows], 0)
    step = eliminate(info + jnp.where(rid == cid, 1.0, 0.0), states, right)
    if rows < lanes:
        step = jnp.concatenate([step, jnp.zeros((lanes - rows, LANES), F32)], 0)
    inc_ref[...] = step.T[:1, :states]


def solve_in_members(total, gram_ref, states_ref, factor_ref, info_ref, grad_ref, inc_ref):
    states = states_ref.shape[2]
    scale = 1.0 / (total - 1)
    rows, lanes = up(states, SUB), up(states, LANES)
    height = gram_ref.shape[0] - SUB
    packed, force = gram_ref[:height], gram_ref[height:height + 1]
    low = lax.broadcasted_iota(jnp.int32, packed.shape, 1) < total
    rolled = pltpu.roll(packed, total, 1)
    gram = jnp.concatenate([jnp.where(low, packed, rolled), jnp.where(low, rolled, packed)], 0)
    left = lax.broadcasted_iota(jnp.int32, (total, LANES), 1) < total
    factor = factor_ref[...]
    right = jnp.sum(jnp.where(left, factor * force, 0.0), axis=1, keepdims=True)
    right = jnp.broadcast_to(right, factor.shape)

    u0, u1, u2 = split3(factor)
    g0, g1, g2 = split3(gram)
    mixed = dots((jnp.concatenate([u0, u1], 1), jnp.concatenate([g0, g1, g0, g1], 0)),
                 (jnp.where(left, u0, u2), jnp.concatenate([g2, g0], 0)))
    m0, m1, m2 = split3(mixed)
    pad = jnp.zeros((LANES - total, LANES), BF16)
    pair = jnp.concatenate([jnp.where(left, u0, u1), pad], 0)
    last = jnp.concatenate([jnp.where(left, u2, u0), pad], 0)
    dims = (((1,), (1,)), ((), ()))
    system = (lax.dot_general(jnp.concatenate([m0, m1], 1), jnp.concatenate([pair, pair], 1), dims,
                              preferred_element_type=F32)
              + lax.dot_general(jnp.where(left, m0, m2), last, dims, preferred_element_type=F32)) * (scale * scale)
    rid = lax.broadcasted_iota(jnp.int32, system.shape, 0)
    cid = lax.broadcasted_iota(jnp.int32, system.shape, 1)
    step = eliminate(system + jnp.where(rid == cid, 1.0, 0.0), total, right)

    anom = states_ref[...].astype(F32).reshape(total, states)
    anom = jnp.concatenate([anom, jnp.zeros((total, lanes - states), F32)], 1)
    twice = jnp.concatenate([anom, anom], 0)
    once = jnp.concatenate([anom, jnp.zeros_like(anom)], 0).astype(BF16)
    f0, f1, f2 = split3(jnp.broadcast_to(force, (2 * SUB, LANES)))
    gradient = (dots((f2, once), (jnp.where(left[:2 * SUB], f0, f1), twice.astype(BF16))) * scale)[:1]
    grad_ref[...] = gradient[:, :states]
    moved = dots((m2, once), (jnp.where(left, m0, m1), twice.astype(BF16))) * (scale * scale * scale)
    inc_ref[...] = (gradient - jnp.sum(jnp.concatenate([step] * (lanes // LANES), 1) * moved,
                                       axis=0, keepdims=True))[:, :states]
    across_states = twice.T[:rows].astype(BF16)
    outer = dots((across_states, jnp.concatenate([g2, jnp.zeros_like(g2)], 0)),
                 (across_states, jnp.concatenate([g0, g1], 0)))
    h0, h1, h2 = split3(outer)
    left = lax.broadcasted_iota(jnp.int32, outer.shape, 1) < total
    info = dots((h2, once), (jnp.where(left, h0, h1), twice.astype(BF16))) * (scale * scale)
    info_ref[:, 0, :] = info[:states, :states]


def shards(state_anom, radiance_anom, inv_noise, innovation, valid_count):
    n_mem, n_chan = lax.axis_size("mem"), lax.axis_size("chan")
    members, states = state_anom.shape[1:]
    width = radiance_anom.shape[2]
    total = members * n_mem
    in_members = total <= states and 2 * total == LANES
    columns = LANES if in_members else total
    height = total * total // columns
    vmem, far = pl.BlockSpec(memory_space=pltpu.VMEM), pl.BlockSpec(memory_space=pltpu.HBM)
    dma = pltpu.SemaphoreType.DMA
    factor = () if not in_members else (jax.ShapeDtypeStruct((total, up(total, LANES)), F32),)
    valid_count, state_anom, radiance_anom, inv_noise, innovation = (pltpu.with_memory_space_constraint(x, pltpu.HBM) for x in (valid_count, state_anom, radiance_anom, inv_noise, innovation))
    gram, own_states, *factors = pl.pallas_call(
        functools.partial(gram_kernel, n_mem, n_chan, PARTS),
        out_shape=(jax.ShapeDtypeStruct((height + SUB, columns), F32),
                   jax.ShapeDtypeStruct((n_mem, members, states), BF16)) + factor,
        in_specs=[far] * 5,
        out_specs=(vmem,) * (2 + len(factor)),
        scratch_shapes=[
            pltpu.SMEM(valid_count.shape, jnp.int32),
            pltpu.VMEM((n_mem, members, width), BF16),
            pltpu.VMEM((n_mem, members, states), BF16),
            pltpu.VMEM((width,), F32),
            pltpu.VMEM(innovation.shape, F32),
            pltpu.VMEM((n_mem, members, width), BF16),
            pltpu.VMEM((n_mem, members, states), BF16),
            pltpu.VMEM((n_chan, height + SUB, columns), F32),
            dma((5,)), dma((PARTS, 2)), dma((2,)), dma((max(n_mem // 2 // n_chan, 1), 2)), dma((2,)), dma((2,)),
        ],
        compiler_params=pltpu.CompilerParams(
            collective_id=0, has_side_effects=True, vmem_limit_bytes=24 * MIB),
    )(valid_count, state_anom, radiance_anom, inv_noise, innovation)
    information, gradient, increment = pl.pallas_call(
        functools.partial(solve_in_members if in_members else solve_in_states, total),
        out_shape=(jax.ShapeDtypeStruct((states, 1, states), F32),
                   jax.ShapeDtypeStruct((1, states), F32),
                   jax.ShapeDtypeStruct((1, states), F32)),
        in_specs=[vmem] * (2 + len(factor)),
        out_specs=(vmem, vmem, vmem),
        compiler_params=pltpu.CompilerParams(vmem_limit_bytes=24 * MIB),
    )(gram, own_states, *factors)
    return information.transpose(1, 0, 2), gradient, increment


def solution(mesh):
    in_specs = (P(None, "mem", None), P(None, "mem", "chan"), P("chan"), P(None, "chan"), P())
    out_specs = (P("mem", None, None), P("mem", None), P("mem", None))
    return jax.shard_map(shards, mesh=mesh, in_specs=in_specs, out_specs=out_specs, check_vma=False)
```

```python
import functools
import jax
import jax.numpy as jnp
from jax import lax
from jax.experimental import pallas as pl
from jax.experimental.pallas import tpu as pltpu
from jax.sharding import PartitionSpec as P

F32, BF16 = jnp.float32, jnp.bfloat16
LANES, SUB = 128, 8
PARTS = 1
STEP = 16
ROUNDING = 2.0 ** -20
MIB = 1024 * 1024


def up(x, to):
    return -(-x // to) * to


def split2(x):
    a = x.astype(BF16)
    return a, (x - a.astype(F32)).astype(BF16)


def split3(x):
    a = x.astype(BF16)
    return (a,) + split2(x - a.astype(F32))


def pieces(width, count):
    tiles = width // LANES
    marks = [(tiles - tiles * i // count) * LANES for i in range(count, 0, -1)] + [width]
    return list(zip(marks[:-1], marks[1:]))


def partner(me, k, n):
    if n & (n - 1):
        return lax.rem(me + k, n)
    other, bit = me, 1
    while bit < n:
        other = other + (k // bit % 2) * bit * (1 - 2 * (me // bit % 2))
        bit *= 2
    return other


def cholesky_rows(square, total):
    lanes = square.shape[1]
    rid8 = lax.broadcasted_iota(jnp.int32, (SUB, lanes), 0)
    cid = lax.broadcasted_iota(jnp.int32, square.shape, 1)
    rid = lax.broadcasted_iota(jnp.int32, square.shape, 0)
    least = jnp.sum(jnp.where(cid == rid, square, 0.0), axis=1, keepdims=True) * ROUNDING
    least = jnp.broadcast_to(least, square.shape)
    live, upper = square, []
    for p in range(0, total, SUB):
        steps = min(SUB, total - p)
        cols = [jnp.broadcast_to(live[:, p + j:p + j + 1], live.shape) for j in range(steps)]
        block, below = live[:SUB], live[SUB:]
        rows = jnp.zeros((SUB, lanes), F32)
        for j in range(steps):
            pivot = cols[j][j:j + 1]
            inverse = jnp.where(pivot > least[p + j:p + j + 1], lax.rsqrt(pivot), 0.0)
            column = cols[j] * inverse
            row = block[j:j + 1] * inverse
            rows = jnp.where(rid8 == j, jnp.broadcast_to(row, rows.shape), rows)
            for later in range(j + 1, steps):
                cols[later] = cols[later] - column * (cols[later][j:j + 1] * inverse)
            block = block - column[:SUB] * row
            if p + SUB < total:
                below = below - column[SUB:] * row
        lane = lax.broadcasted_iota(jnp.int32, (SUB, lanes), 1)
        upper.append(jnp.where(lane >= rid8 + p, rows, 0.0))
        live = below
    return jnp.concatenate(upper, 0)


def stack_factor(factor, total):
    u0, u1, u2 = (piece.astype(F32) for piece in split3(factor))
    slot = lax.broadcasted_iota(jnp.int32, factor.shape, 1) // (total // 2)

    def placed(*those):
        out = []
        for side in range(2):
            tile = jnp.zeros(factor.shape, F32)
            for i, piece in enumerate(those):
                shift = (i - side) * (total // 2) % LANES
                tile = jnp.where(slot == i, pltpu.roll(piece, shift, 1) if shift else piece, tile)
            out.append(tile)
        return jnp.concatenate(out, 0)

    return placed(u0, u0, u1, u1), placed(u0, u2)


def gram_kernel(n_mem, n_chan, parts_of_slab, count_hbm, state_hbm, rad_hbm, noise_hbm, innov_hbm,
                gram_ref, states_ref, *rest):
    factor_refs = rest[:-14]
    (count, mine, mine_states, noise, innov, held, held_states, parts,
     local_sem, mem_sem, near_sem, far_sem, relay_sem, chan_sem) = rest[-14:]
    me, slab = lax.axis_index("mem"), lax.axis_index("chan")
    members, width = rad_hbm.shape[1:]
    states = state_hbm.shape[2]
    total = n_mem * members
    columns = parts.shape[2]
    height = parts.shape[1] - SUB
    sent = height + (1 if columns == LANES else SUB)

    barrier = pltpu.get_barrier_semaphore()
    def greet(rounds):
        for k in rounds:
            pl.semaphore_signal(barrier, inc=1, device_id={"mem": partner(me, k, n_mem)})

    local = [
        pltpu.make_async_copy(src, dst, local_sem.at[i])
        for i, (src, dst) in enumerate((
            (state_hbm, mine_states), (rad_hbm, mine), (count_hbm, count), (noise_hbm, noise), (innov_hbm, innov)))
    ]
    greet(range(n_mem - 1, n_mem // 2 - 1, -1))
    local[0].start()
    local[1].start()
    greet(range(n_mem // 2 - 1, 0, -1))
    for k in range(1, n_chan):
        pl.semaphore_signal(barrier, inc=1, device_id={"chan": partner(slab, k, n_chan)})
    for copy in local[2:]:
        copy.start()
    for copy in local[:2]:
        copy.wait()
    pl.semaphore_wait(barrier, n_mem - 1 + n_chan - 1)

    near = n_mem // 2
    shared = near // n_chan if n_mem & (n_mem - 1) == 0 and near % n_chan == 0 else 0
    direct = near if shared else n_mem

    def state_copy(k, sems):
        peer = partner(me, k, n_mem)
        return pltpu.make_async_remote_copy(
            src_ref=mine_states.at[peer], dst_ref=held_states.at[k],
            send_sem=sems.at[0], recv_sem=sems.at[1], device_id={"mem": peer})

    def blocks(source, target, sems):
        return pltpu.make_async_remote_copy(
            src_ref=source, dst_ref=target, send_sem=sems.at[0], recv_sem=sems.at[1],
            device_id={"mem": partner(me, 1, n_mem)})

    far = [state_copy(near + i * n_chan + slab, far_sem.at[i]) for i in range(shared)]
    for copy in far:
        copy.start()
    for k in range(direct - 1, 0, -1):
        state_copy(k, near_sem).start()
    all_states = blocks(mine_states.at[1:direct], held_states.at[1:direct], near_sem)
    cuts = pieces(width, parts_of_slab)
    rounds = sorted(range(1, n_mem), key=lambda k: (k < near, k // 2 % 2, -k))
    sends = []
    for c, (lo, hi) in enumerate(cuts):
        for k in rounds:
            peer = partner(me, k, n_mem)
            pltpu.make_async_remote_copy(
                src_ref=mine.at[peer, :, lo:hi], dst_ref=held.at[k, :, lo:hi],
                send_sem=mem_sem.at[c, 0], recv_sem=mem_sem.at[c, 1], device_id={"mem": peer}).start()
        sends.append(blocks(mine.at[1:, :, lo:hi], held.at[1:, :, lo:hi], mem_sem.at[c]))
    for copy in local[2:]:
        copy.wait()
    slots = slab * width + lax.broadcasted_iota(jnp.int32, (1, width), 1)
    weight = jnp.where(slots < count[me], noise[...].reshape(1, width), 0.0)
    pull = weight * innov[pl.ds(me, 1), :]
    pull = [part.astype(F32) for part in split2(pull)]

    relays = []
    for i, copy in enumerate(far):
        copy.wait_recv()
        k = near + i * n_chan + slab
        for j in range(1, n_chan):
            pltpu.make_async_remote_copy(
                src_ref=held_states.at[k], dst_ref=held_states.at[k], send_sem=relay_sem.at[0],
                recv_sem=relay_sem.at[1], device_id={"chan": partner(slab, j, n_chan)}).start()
    if shared:
        size = shared * (n_chan - 1)
        relays.append(blocks(mine_states.at[:size], held_states.at[:size], relay_sem))
    def whole(own, others, lo, hi):
        parts_of = [own[pl.ds(me, 1), :, lo:hi], others[1:, :, lo:hi]]
        return jnp.concatenate([part.astype(F32).reshape(-1, hi - lo) for part in parts_of], 0)

    row = lax.broadcasted_iota(jnp.int32, (2 * SUB, 1), 0)
    acc = jnp.zeros((2 * total + 2 * SUB, columns), F32)
    step = 2 * LANES
    for (start, stop), copy in zip(cuts, sends):
        copy.wait_recv()
        for lo in range(start, stop, step):
            hi = min(lo + step, stop)
            block = whole(mine, held, lo, hi)
            first, second = split2(block * weight[:, lo:hi])
            tail = jnp.where(row == 0, pull[0][:, lo:hi], jnp.where(row == 1, pull[1][:, lo:hi], 0.0)).astype(BF16)
            block = jnp.concatenate([block.astype(BF16)] * (columns // total), 0)
            acc += lax.dot_general(jnp.concatenate([first, second, tail], 0), block, (((1,), (1,)), ((), ())),
                                   preferred_element_type=F32)
    square = acc[:total] + acc[total:2 * total]
    if columns > total:
        lane = lax.broadcasted_iota(jnp.int32, (height, columns), 1)
        square = jnp.where(lane < total, square[:height], square[height:])
    parts[slab, :height] = square
    parts[slab, height:] = jnp.broadcast_to(acc[2 * total:2 * total + 1] + acc[2 * total + 1:2 * total + 2],
                                            (SUB, columns))
    for k in range(1, n_chan):
        pltpu.make_async_remote_copy(
            src_ref=parts.at[slab, :sent], dst_ref=parts.at[slab, :sent], send_sem=chan_sem.at[0], recv_sem=chan_sem.at[1],
            device_id={"chan": partner(slab, k, n_chan)}).start()
    all_states.wait_recv()
    for copy in relays:
        copy.wait_recv()
    states_ref[pl.ds(0, 1)] = mine_states[pl.ds(me, 1)]
    states_ref[1:] = held_states[1:]
    if factor_refs:
        anom = whole(mine_states, held_states, 0, states)
        anom = jnp.concatenate([anom, jnp.zeros((total, up(states, LANES) - states), F32)], 1)
        tall = jnp.concatenate([anom, jnp.zeros((up(total, LANES) - total, anom.shape[1]), F32)], 0)
        square = lax.dot_general(anom.astype(BF16), tall.astype(BF16), (((1,), (1,)), ((), ())),
                                 preferred_element_type=F32)
        factor = cholesky_rows(square, total)
        factor_refs[0][...] = factor + pltpu.roll(factor, total, 1)
        stacked = stack_factor(factor, total)
        for i, tile in enumerate(stacked):
            factor_refs[1][:, i * LANES:(i + 1) * LANES] = tile
    for copy in [all_states] + far + sends + relays:
        copy.wait_send()
    arrived = parts.at[:n_chan - 1, :sent]
    blocks(arrived, arrived, chan_sem).wait()
    for rows in (slice(0, height), slice(height, height + 1)):
        summed = parts[0, rows]
        for k in range(1, n_chan):
            summed = summed + parts[k, rows]
        gram_ref[rows] = summed


def eliminate(system, order):
    rows, lanes = system.shape
    rid = lax.broadcasted_iota(jnp.int32, (SUB, LANES), 0)

    def wide(piece, tiles):
        return piece if tiles == 1 else jnp.concatenate([piece] * tiles, 1)

    for p in range(0, order, STEP):
        steps = min(STEP, order - p)
        size = up(steps, SUB)
        base = p // LANES * LANES
        tiles = (lanes - base) // LANES
        live = system[:, base:]
        at = p - base
        final = p + STEP >= order

        def others(x):
            kept = ([x[:p]] if p else []) + ([x[p + size:]] if p + size < rows else [])
            return (jnp.concatenate(kept, 0) if len(kept) > 1 else kept[0]) if kept else None

        def joined(inner, outer):
            out = ([outer[:p]] if p else []) + inner + ([outer[p:]] if p + size < rows else [])
            return jnp.concatenate(out, 0) if len(out) > 1 else out[0]

        block = [live[p + i:p + i + SUB] for i in range(0, size, SUB)]
        cols = [[jnp.broadcast_to(b[:, at + j:at + j + 1], (SUB, LANES)) for b in block] for j in range(steps)]
        if final:
            cols.append([across(b, order - base) for b in block])
        far = others(live)
        if far is not None:
            factors = [across(far, at + j) for j in range(steps)]
            far_right = across(far, order - base) if final else None
        scales = [jnp.ones((SUB, LANES), F32)] * len(block)
        for j in range(steps):
            home, k = divmod(j, SUB)
            inverse = 1.0 / cols[j][home][k:k + 1, :]
            scales[home] = jnp.where(rid == k, inverse, scales[home])
            factor = list(cols[j])
            factor[home] = jnp.where(rid == k, 0.0, factor[home])
            for later in range(j + 1, len(cols)):
                c = cols[later]
                scale = c[home][k:k + 1, :] * inverse
                cols[later] = [c[i] - factor[i] * scale for i in range(len(c))]
            pivot_row = block[home][k:k + 1, :] * wide(inverse, tiles)
            block = [b - wide(factor[i], tiles) * pivot_row for i, b in enumerate(block)]
        if final:
            solved = [c * s for c, s in zip(cols[steps], scales)]
            if far is not None:
                terms = [factors[j] * solved[j // SUB][j % SUB:j % SUB + 1, :] for j in range(steps)]
                far_right = far_right - sum(sum(terms[i::4][1:], terms[i]) for i in range(min(4, steps)))
            return joined(solved, far_right)
        block = [b * wide(s, tiles) for b, s in zip(block, scales)]
        if far is not None:
            for j in range(steps):
                far = far - wide(factors[j], tiles) * block[j // SUB][j % SUB:j % SUB + 1, :]
        live = joined(block, far)
        system = live if base == 0 else jnp.concatenate([system[:, :base], live], 1)


def across(x, lane):
    return jnp.broadcast_to(x[:, lane:lane + 1], (x.shape[0], LANES))


def dots(*pairs):
    return functools.reduce(lambda a, b: a + b, [jnp.dot(a, b, preferred_element_type=F32) for a, b in pairs])


def solve_in_states(total, gram_ref, states_ref, info_ref, grad_ref, inc_ref):
    states = states_ref.shape[2]
    scale = 1.0 / (total - 1)
    rows, lanes = up(states, SUB), up(states + 1, LANES)
    anom = states_ref[...].astype(F32).reshape(total, states)
    anom = jnp.concatenate([anom, jnp.zeros((total, lanes - states), F32)], 1)
    gram, force = gram_ref[:total], gram_ref[total:total + 1]
    gradient = jnp.dot(force, anom, precision=lax.Precision.HIGHEST, preferred_element_type=F32) * scale
    grad_ref[...] = gradient[:, :states]
    deep = anom.astype(BF16)
    turned = anom.T[:rows].astype(BF16)
    mixed = dots(*((turned, g) for g in split3(gram)[::-1]))
    info = dots(*((m, deep) for m in split3(mixed)[::-1])) * (scale * scale)
    info_ref[:, 0, :] = info[:states, :states]
    rid = lax.broadcasted_iota(jnp.int32, (rows, lanes), 0)
    cid = lax.broadcasted_iota(jnp.int32, (rows, lanes), 1)
    wide_right = jnp.broadcast_to(jnp.broadcast_to(gradient, (SUB, lanes)).T[:rows, :1], (rows, lanes))
    step = eliminate(jnp.where(cid == states, wide_right, info + jnp.where(rid == cid, 1.0, 0.0)), states)
    if rows < lanes:
        step = jnp.concatenate([step, jnp.zeros((lanes - rows, LANES), F32)], 0)
    inc_ref[...] = step.T[:1, :states]


def solve_in_members(total, gram_ref, states_ref, factor_ref, stacked_ref, info_ref, grad_ref, inc_ref):
    states = states_ref.shape[2]
    scale = 1.0 / (total - 1)
    rows, lanes = up(states, SUB), up(states, LANES)
    height = gram_ref.shape[0] - SUB
    packed, force = gram_ref[:height], gram_ref[height:height + 1]
    low = lax.broadcasted_iota(jnp.int32, packed.shape, 1) < total
    rolled = pltpu.roll(packed, total, 1)
    gram = jnp.concatenate([jnp.where(low, packed, rolled), jnp.where(low, rolled, packed)], 0)
    left = lax.broadcasted_iota(jnp.int32, (total, LANES), 1) < total
    factor = factor_ref[...]
    right = jnp.sum(jnp.where(left, factor * force, 0.0), axis=1, keepdims=True)
    right = jnp.broadcast_to(right, factor.shape)

    u0, u1, u2 = split3(factor)
    g0, g1, g2 = split3(gram)
    p0, p1, p2 = split3(packed)
    deep = jnp.concatenate([p0, p1, p0, p1, p2, p0, jnp.zeros((2 * LANES - 6 * height, LANES), BF16)], 0)
    halves = jnp.dot(stacked_ref[...].astype(BF16), deep, preferred_element_type=F32)
    m0, m1, m2 = split3(jnp.where(left, halves[:total], halves[total:]))
    pad = jnp.zeros((LANES - total, LANES), BF16)
    dims = (((1,), (1,)), ((), ()))
    system = sum(
        lax.dot_general(jnp.concatenate(a, 1), jnp.concatenate([jnp.concatenate(b, 1), jnp.concatenate([pad, pad], 1)], 0),
                        dims, preferred_element_type=F32)
        for a, b in (((m0, m2), (u2, u0)), ((m0, m1), (u1, u1)), ((m0, m1), (u0, u0)))) * (scale * scale)
    rid = lax.broadcasted_iota(jnp.int32, system.shape, 0)
    cid = lax.broadcasted_iota(jnp.int32, system.shape, 1)
    step = eliminate(jnp.where(cid == total, right, system + jnp.where(rid == cid, 1.0, 0.0)), total)

    anom = states_ref[...].astype(F32).reshape(total, states)
    anom = jnp.concatenate([anom, jnp.zeros((total, lanes - states), F32)], 1)
    twice = jnp.concatenate([anom, anom], 0)
    once = jnp.concatenate([anom, jnp.zeros_like(anom)], 0).astype(BF16)
    f0, f1, f2 = split3(jnp.broadcast_to(force, (2 * SUB, LANES)))
    gradient = (dots((f2, once), (jnp.where(left[:2 * SUB], f0, f1), twice.astype(BF16))) * scale)[:1]
    grad_ref[...] = gradient[:, :states]
    moved = dots(*((m, twice.astype(BF16)) for m in (m2, m1, m0))) * (scale * scale * scale)
    inc_ref[...] = (gradient - jnp.sum(jnp.concatenate([step] * (lanes // LANES), 1) * moved,
                                       axis=0, keepdims=True))[:, :states]
    across_states = twice.T[:rows].astype(BF16)
    outer = dots((across_states, jnp.concatenate([g2, jnp.zeros_like(g2)], 0)),
                 (across_states, jnp.concatenate([g0, g1], 0)))
    h0, h1, h2 = split3(outer * (scale * scale))
    left = lax.broadcasted_iota(jnp.int32, outer.shape, 1) < total
    info = dots((h2, once), (jnp.where(left, h0, h1), twice.astype(BF16)))
    info_ref[:, 0, :] = info[:states, :states]


def shards(state_anom, radiance_anom, inv_noise, innovation, valid_count):
    n_mem, n_chan = lax.axis_size("mem"), lax.axis_size("chan")
    members, states = state_anom.shape[1:]
    width = radiance_anom.shape[2]
    total = members * n_mem
    in_members = total <= states and 2 * total == LANES
    columns = LANES if in_members else total
    height = total * total // columns
    vmem, far = pl.BlockSpec(memory_space=pltpu.VMEM), pl.BlockSpec(memory_space=pltpu.HBM)
    dma = pltpu.SemaphoreType.DMA
    factor = () if not in_members else (jax.ShapeDtypeStruct((total, LANES), F32),
                                        jax.ShapeDtypeStruct((2 * total, 2 * LANES), F32))
    valid_count, state_anom, radiance_anom, inv_noise, innovation = (pltpu.with_memory_space_constraint(x, pltpu.HBM) for x in (valid_count, state_anom, radiance_anom, inv_noise, innovation))
    gram, own_states, *factors = pl.pallas_call(
        functools.partial(gram_kernel, n_mem, n_chan, PARTS),
        out_shape=(jax.ShapeDtypeStruct((height + SUB, columns), F32),
                   jax.ShapeDtypeStruct((n_mem, members, states), BF16)) + factor,
        in_specs=[far] * 5,
        out_specs=(vmem,) * (2 + len(factor)),
        scratch_shapes=[
            pltpu.SMEM(valid_count.shape, jnp.int32),
            pltpu.VMEM((n_mem, members, width), BF16),
            pltpu.VMEM((n_mem, members, states), BF16),
            pltpu.VMEM((width,), F32),
            pltpu.VMEM(innovation.shape, F32),
            pltpu.VMEM((n_mem, members, width), BF16),
            pltpu.VMEM((n_mem, members, states), BF16),
            pltpu.VMEM((n_chan, height + SUB, columns), F32),
            dma((5,)), dma((PARTS, 2)), dma((2,)), dma((max(n_mem // 2 // n_chan, 1), 2)), dma((2,)), dma((2,)),
        ],
        compiler_params=pltpu.CompilerParams(
            collective_id=0, has_side_effects=True, vmem_limit_bytes=24 * MIB),
    )(valid_count, state_anom, radiance_anom, inv_noise, innovation)
    information, gradient, increment = pl.pallas_call(
        functools.partial(solve_in_members if in_members else solve_in_states, total),
        out_shape=(jax.ShapeDtypeStruct((states, 1, states), F32),
                   jax.ShapeDtypeStruct((1, states), F32),
                   jax.ShapeDtypeStruct((1, states), F32)),
        in_specs=[vmem] * (2 + len(factor)),
        out_specs=(vmem, vmem, vmem),
        compiler_params=pltpu.CompilerParams(vmem_limit_bytes=24 * MIB),
    )(gram, own_states, *factors)
    return information.transpose(1, 0, 2), gradient, increment


def solution(mesh):
    in_specs = (P(None, "mem", None), P(None, "mem", "chan"), P("chan"), P(None, "chan"), P())
    out_specs = (P("mem", None, None), P("mem", None), P("mem", None))
    return jax.shard_map(shards, mesh=mesh, in_specs=in_specs, out_specs=out_specs, check_vma=False)
```

```python
import functools
import jax
import jax.numpy as jnp
from jax import lax
from jax.experimental import pallas as pl
from jax.experimental.pallas import tpu as pltpu
from jax.sharding import PartitionSpec as P

F32, BF16 = jnp.float32, jnp.bfloat16
LANES, SUB = 128, 8
PARTS = 1
STEP = 16
ROUNDING = 2.0 ** -20
MIB = 1024 * 1024


def up(x, to):
    return -(-x // to) * to


def split2(x):
    a = x.astype(BF16)
    return a, (x - a.astype(F32)).astype(BF16)


def split3(x):
    a = x.astype(BF16)
    return (a,) + split2(x - a.astype(F32))


def pieces(width, count):
    tiles = width // LANES
    marks = [(tiles - tiles * i // count) * LANES for i in range(count, 0, -1)] + [width]
    return list(zip(marks[:-1], marks[1:]))


def partner(me, k, n):
    if n & (n - 1):
        return lax.rem(me + k, n)
    other, bit = me, 1
    while bit < n:
        other = other + (k // bit % 2) * bit * (1 - 2 * (me // bit % 2))
        bit *= 2
    return other


def cholesky_rows(square, total):
    lanes = square.shape[1]
    rid8 = lax.broadcasted_iota(jnp.int32, (SUB, lanes), 0)
    cid = lax.broadcasted_iota(jnp.int32, square.shape, 1)
    rid = lax.broadcasted_iota(jnp.int32, square.shape, 0)
    least = jnp.sum(jnp.where(cid == rid, square, 0.0), axis=1, keepdims=True) * ROUNDING
    least = jnp.broadcast_to(least, square.shape)
    live, upper = square, []
    for p in range(0, total, SUB):
        steps = min(SUB, total - p)
        cols = [jnp.broadcast_to(live[:, p + j:p + j + 1], live.shape) for j in range(steps)]
        block, below = live[:SUB], live[SUB:]
        rows = jnp.zeros((SUB, lanes), F32)
        for j in range(steps):
            pivot = cols[j][j:j + 1]
            inverse = jnp.where(pivot > least[p + j:p + j + 1], lax.rsqrt(pivot), 0.0)
            column = cols[j] * inverse
            row = block[j:j + 1] * inverse
            rows = jnp.where(rid8 == j, jnp.broadcast_to(row, rows.shape), rows)
            for later in range(j + 1, steps):
                cols[later] = cols[later] - column * (cols[later][j:j + 1] * inverse)
            block = block - column[:SUB] * row
            if p + SUB < total:
                below = below - column[SUB:] * row
        lane = lax.broadcasted_iota(jnp.int32, (SUB, lanes), 1)
        upper.append(jnp.where(lane >= rid8 + p, rows, 0.0))
        live = below
    return jnp.concatenate(upper, 0)


def stack_factor(factor, total):
    u0, u1, u2 = (piece.astype(F32) for piece in split3(factor))
    slot = lax.broadcasted_iota(jnp.int32, factor.shape, 1) // (total // 2)

    def placed(*those):
        out = []
        for side in range(2):
            tile = jnp.zeros(factor.shape, F32)
            for i, piece in enumerate(those):
                shift = (i - side) * (total // 2) % LANES
                tile = jnp.where(slot == i, pltpu.roll(piece, shift, 1) if shift else piece, tile)
            out.append(tile)
        return jnp.concatenate(out, 0)

    return placed(u0, u0, u1, u1), placed(u0, u2)


def gram_kernel(n_mem, n_chan, parts_of_slab, count_hbm, state_hbm, rad_hbm, noise_hbm, innov_hbm,
                gram_ref, states_ref, *rest):
    factor_refs = rest[:-14]
    (count, mine, mine_states, noise, innov, held, held_states, parts,
     local_sem, mem_sem, near_sem, far_sem, relay_sem, chan_sem) = rest[-14:]
    me, slab = lax.axis_index("mem"), lax.axis_index("chan")
    members, width = rad_hbm.shape[1:]
    states = state_hbm.shape[2]
    total = n_mem * members
    columns = parts.shape[2]
    height = parts.shape[1] - SUB
    sent = height + (1 if columns == LANES else SUB)

    barrier = pltpu.get_barrier_semaphore()
    def greet(rounds):
        for k in rounds:
            pl.semaphore_signal(barrier, inc=1, device_id={"mem": partner(me, k, n_mem)})

    local = [
        pltpu.make_async_copy(src, dst, local_sem.at[i])
        for i, (src, dst) in enumerate((
            (state_hbm, mine_states), (rad_hbm, mine), (count_hbm, count), (noise_hbm, noise), (innov_hbm, innov)))
    ]
    greet(range(n_mem - 1, n_mem // 2 - 1, -1))
    local[0].start()
    local[1].start()
    greet(range(n_mem // 2 - 1, 0, -1))
    for k in range(1, n_chan):
        pl.semaphore_signal(barrier, inc=1, device_id={"chan": partner(slab, k, n_chan)})
    for copy in local[2:]:
        copy.start()
    for copy in local[:2]:
        copy.wait()
    pl.semaphore_wait(barrier, n_mem - 1 + n_chan - 1)

    near = n_mem // 2
    shared = near // n_chan if n_mem & (n_mem - 1) == 0 and near % n_chan == 0 else 0
    direct = near if shared else n_mem

    def state_copy(k, sems):
        peer = partner(me, k, n_mem)
        return pltpu.make_async_remote_copy(
            src_ref=mine_states.at[peer], dst_ref=held_states.at[k],
            send_sem=sems.at[0], recv_sem=sems.at[1], device_id={"mem": peer})

    def blocks(source, target, sems):
        return pltpu.make_async_remote_copy(
            src_ref=source, dst_ref=target, send_sem=sems.at[0], recv_sem=sems.at[1],
            device_id={"mem": partner(me, 1, n_mem)})

    far = [state_copy(near + i * n_chan + slab, far_sem.at[i]) for i in range(shared)]
    for copy in far:
        copy.start()
    for k in range(direct - 1, 0, -1):
        state_copy(k, near_sem).start()
    all_states = blocks(mine_states.at[1:direct], held_states.at[1:direct], near_sem)
    cuts = pieces(width, parts_of_slab)
    rounds = sorted(range(1, n_mem), key=lambda k: (k < near, k // 2 % 2, -k))
    sends = []
    for c, (lo, hi) in enumerate(cuts):
        for k in rounds:
            peer = partner(me, k, n_mem)
            pltpu.make_async_remote_copy(
                src_ref=mine.at[peer, :, lo:hi], dst_ref=held.at[k, :, lo:hi],
                send_sem=mem_sem.at[c, 0], recv_sem=mem_sem.at[c, 1], device_id={"mem": peer}).start()
        sends.append(blocks(mine.at[1:, :, lo:hi], held.at[1:, :, lo:hi], mem_sem.at[c]))
    for copy in local[2:]:
        copy.wait()
    slots = slab * width + lax.broadcasted_iota(jnp.int32, (1, width), 1)
    weight = jnp.where(slots < count[me], noise[...].reshape(1, width), 0.0)
    pull = weight * innov[pl.ds(me, 1), :]
    pull = [part.astype(F32) for part in split3(pull)]

    relays = []
    for i, copy in enumerate(far):
        copy.wait_recv()
        k = near + i * n_chan + slab
        for j in range(1, n_chan):
            pltpu.make_async_remote_copy(
                src_ref=held_states.at[k], dst_ref=held_states.at[k], send_sem=relay_sem.at[0],
                recv_sem=relay_sem.at[1], device_id={"chan": partner(slab, j, n_chan)}).start()
    if shared:
        size = shared * (n_chan - 1)
        relays.append(blocks(mine_states.at[:size], held_states.at[:size], relay_sem))
    def whole(own, others, lo, hi):
        parts_of = [own[pl.ds(me, 1), :, lo:hi], others[1:, :, lo:hi]]
        return jnp.concatenate([part.astype(F32).reshape(-1, hi - lo) for part in parts_of], 0)

    row = lax.broadcasted_iota(jnp.int32, (2 * SUB, 1), 0)
    acc = jnp.zeros((2 * total + 2 * SUB, columns), F32)
    step = 2 * LANES
    for (start, stop), copy in zip(cuts, sends):
        copy.wait_recv()
        for lo in range(start, stop, step):
            hi = min(lo + step, stop)
            block = whole(mine, held, lo, hi)
            first, second = split2(block * weight[:, lo:hi])
            tail = sum(jnp.where(row == i, part[:, lo:hi], 0.0) for i, part in enumerate(pull)).astype(BF16)
            block = jnp.concatenate([block.astype(BF16)] * (columns // total), 0)
            acc += lax.dot_general(jnp.concatenate([first, second, tail], 0), block, (((1,), (1,)), ((), ())),
                                   preferred_element_type=F32)
    square = acc[:total] + acc[total:2 * total]
    if columns > total:
        lane = lax.broadcasted_iota(jnp.int32, (height, columns), 1)
        square = jnp.where(lane < total, square[:height], square[height:])
    parts[slab, :height] = square
    parts[slab, height:] = jnp.broadcast_to(sum(acc[2 * total + i:2 * total + i + 1] for i in range(len(pull))[::-1]),
                                            (SUB, columns))
    for k in range(1, n_chan):
        pltpu.make_async_remote_copy(
            src_ref=parts.at[slab, :sent], dst_ref=parts.at[slab, :sent], send_sem=chan_sem.at[0], recv_sem=chan_sem.at[1],
            device_id={"chan": partner(slab, k, n_chan)}).start()
    all_states.wait_recv()
    for copy in relays:
        copy.wait_recv()
    states_ref[pl.ds(0, 1)] = mine_states[pl.ds(me, 1)]
    states_ref[1:] = held_states[1:]
    if factor_refs:
        anom = whole(mine_states, held_states, 0, states)
        anom = jnp.concatenate([anom, jnp.zeros((total, up(states, LANES) - states), F32)], 1)
        tall = jnp.concatenate([anom, jnp.zeros((up(total, LANES) - total, anom.shape[1]), F32)], 0)
        square = lax.dot_general(anom.astype(BF16), tall.astype(BF16), (((1,), (1,)), ((), ())),
                                 preferred_element_type=F32)
        rows = cholesky_rows(jnp.concatenate([square, anom], 1), total)
        factor = rows[:, :LANES]
        factor_refs[2][...] = rows[:, LANES:]
        factor_refs[0][...] = factor + pltpu.roll(factor, total, 1)
        stacked = stack_factor(factor, total)
        for i, tile in enumerate(stacked):
            factor_refs[1][:, i * LANES:(i + 1) * LANES] = tile
    for copy in [all_states] + far + sends + relays:
        copy.wait_send()
    arrived = parts.at[:n_chan - 1, :sent]
    blocks(arrived, arrived, chan_sem).wait()
    for rows in (slice(0, height), slice(height, height + 1)):
        summed = parts[0, rows]
        for k in range(1, n_chan):
            summed = summed + parts[k, rows]
        gram_ref[rows] = summed


def eliminate(system, order):
    rows, lanes = system.shape
    rid = lax.broadcasted_iota(jnp.int32, (SUB, LANES), 0)

    def wide(piece, tiles):
        return piece if tiles == 1 else jnp.concatenate([piece] * tiles, 1)

    for p in range(0, order, STEP):
        steps = min(STEP, order - p)
        size = up(steps, SUB)
        base = p // LANES * LANES
        tiles = (lanes - base) // LANES
        live = system[:, base:]
        at = p - base
        final = p + STEP >= order

        def others(x):
            kept = ([x[:p]] if p else []) + ([x[p + size:]] if p + size < rows else [])
            return (jnp.concatenate(kept, 0) if len(kept) > 1 else kept[0]) if kept else None

        def joined(inner, outer):
            out = ([outer[:p]] if p else []) + inner + ([outer[p:]] if p + size < rows else [])
            return jnp.concatenate(out, 0) if len(out) > 1 else out[0]

        block = [live[p + i:p + i + SUB] for i in range(0, size, SUB)]
        cols = [[jnp.broadcast_to(b[:, at + j:at + j + 1], (SUB, LANES)) for b in block] for j in range(steps)]
        if final:
            cols.append([across(b, order - base) for b in block])
        far = others(live)
        if far is not None:
            factors = [across(far, at + j) for j in range(steps)]
            far_right = across(far, order - base) if final else None
        scales = [jnp.ones((SUB, LANES), F32)] * len(block)
        for j in range(steps):
            home, k = divmod(j, SUB)
            inverse = 1.0 / cols[j][home][k:k + 1, :]
            scales[home] = jnp.where(rid == k, inverse, scales[home])
            factor = list(cols[j])
            factor[home] = jnp.where(rid == k, 0.0, factor[home])
            for later in range(j + 1, len(cols)):
                c = cols[later]
                scale = c[home][k:k + 1, :] * inverse
                cols[later] = [c[i] - factor[i] * scale for i in range(len(c))]
            pivot_row = block[home][k:k + 1, :] * wide(inverse, tiles)
            block = [b - wide(factor[i], tiles) * pivot_row for i, b in enumerate(block)]
        if final:
            solved = [c * s for c, s in zip(cols[steps], scales)]
            if far is not None:
                terms = [factors[j] * solved[j // SUB][j % SUB:j % SUB + 1, :] for j in range(steps)]
                far_right = far_right - sum(sum(terms[i::4][1:], terms[i]) for i in range(min(4, steps)))
            return joined(solved, far_right)
        block = [b * wide(s, tiles) for b, s in zip(block, scales)]
        if far is not None:
            for j in range(steps):
                far = far - wide(factors[j], tiles) * block[j // SUB][j % SUB:j % SUB + 1, :]
        live = joined(block, far)
        system = live if base == 0 else jnp.concatenate([system[:, :base], live], 1)


def across(x, lane):
    return jnp.broadcast_to(x[:, lane:lane + 1], (x.shape[0], LANES))


def dots(*pairs):
    return functools.reduce(lambda a, b: a + b, [jnp.dot(a, b, preferred_element_type=F32) for a, b in pairs])


def solve_in_states(total, gram_ref, states_ref, info_ref, grad_ref, inc_ref):
    states = states_ref.shape[2]
    scale = 1.0 / (total - 1)
    rows, lanes = up(states, SUB), up(states + 1, LANES)
    anom = states_ref[...].astype(F32).reshape(total, states)
    anom = jnp.concatenate([anom, jnp.zeros((total, lanes - states), F32)], 1)
    gram, force = gram_ref[:total], gram_ref[total:total + 1]
    gradient = jnp.dot(force, anom, precision=lax.Precision.HIGHEST, preferred_element_type=F32) * scale
    grad_ref[...] = gradient[:, :states]
    deep = anom.astype(BF16)
    turned = anom.T[:rows].astype(BF16)
    mixed = dots(*((turned, g) for g in split3(gram)[::-1]))
    info = dots(*((m, deep) for m in split3(mixed)[::-1])) * (scale * scale)
    info_ref[:, 0, :] = info[:states, :states]
    rid = lax.broadcasted_iota(jnp.int32, (rows, lanes), 0)
    cid = lax.broadcasted_iota(jnp.int32, (rows, lanes), 1)
    wide_right = jnp.broadcast_to(jnp.broadcast_to(gradient, (SUB, lanes)).T[:rows, :1], (rows, lanes))
    step = eliminate(jnp.where(cid == states, wide_right, info + jnp.where(rid == cid, 1.0, 0.0)), states)
    if rows < lanes:
        step = jnp.concatenate([step, jnp.zeros((lanes - rows, LANES), F32)], 0)
    inc_ref[...] = step.T[:1, :states]


def solve_in_members(total, gram_ref, states_ref, factor_ref, stacked_ref, basis_ref, info_ref, grad_ref, inc_ref):
    states = states_ref.shape[2]
    scale = 1.0 / (total - 1)
    rows, lanes = up(states, SUB), up(states, LANES)
    height = gram_ref.shape[0] - SUB
    packed, force = gram_ref[:height], gram_ref[height:height + 1]
    low = lax.broadcasted_iota(jnp.int32, packed.shape, 1) < total
    rolled = pltpu.roll(packed, total, 1)
    gram = jnp.concatenate([jnp.where(low, packed, rolled), jnp.where(low, rolled, packed)], 0)
    left = lax.broadcasted_iota(jnp.int32, (total, LANES), 1) < total
    factor = factor_ref[...]
    right = jnp.sum(jnp.where(left, factor * force, 0.0), axis=1, keepdims=True)
    right = jnp.broadcast_to(right, factor.shape)

    u0, u1, u2 = split3(factor)
    g0, g1, g2 = split3(gram)
    p0, p1, p2 = split3(packed)
    deep = jnp.concatenate([p0, p1, p0, p1, p2, p0, jnp.zeros((2 * LANES - 6 * height, LANES), BF16)], 0)
    halves = jnp.dot(stacked_ref[...].astype(BF16), deep, preferred_element_type=F32)
    m0, m1, m2 = split3(jnp.where(left, halves[:total], halves[total:]))
    pad = jnp.zeros((LANES - total, LANES), BF16)
    dims = (((1,), (1,)), ((), ()))
    system = sum(
        lax.dot_general(jnp.concatenate(a, 1), jnp.concatenate([jnp.concatenate(b, 1), jnp.concatenate([pad, pad], 1)], 0),
                        dims, preferred_element_type=F32)
        for a, b in (((m0, m2), (u2, u0)), ((m0, m1), (u1, u1)), ((m0, m1), (u0, u0)))) * (scale * scale)
    rid = lax.broadcasted_iota(jnp.int32, system.shape, 0)
    cid = lax.broadcasted_iota(jnp.int32, system.shape, 1)
    step = eliminate(jnp.where(cid == total, right, system + jnp.where(rid == cid, 1.0, 0.0)), total)

    anom = states_ref[...].astype(F32).reshape(total, states)
    anom = jnp.concatenate([anom, jnp.zeros((total, lanes - states), F32)], 1)
    twice = jnp.concatenate([anom, anom], 0)
    once = jnp.concatenate([anom, jnp.zeros_like(anom)], 0).astype(BF16)
    f0, f1, f2 = split3(jnp.broadcast_to(force, (2 * SUB, LANES)))
    gradient = (dots((f2, once), (jnp.where(left[:2 * SUB], f0, f1), twice.astype(BF16))) * scale)[:1]
    grad_ref[...] = gradient[:, :states]
    inc_ref[...] = jnp.sum(jnp.concatenate([step * scale] * (lanes // LANES), 1) * basis_ref[...],
                           axis=0, keepdims=True)[:, :states]
    across_states = twice.T[:rows].astype(BF16)
    outer = dots((across_states, jnp.concatenate([g2, jnp.zeros_like(g2)], 0)),
                 (across_states, jnp.concatenate([g0, g1], 0)))
    h0, h1, h2 = split3(outer * (scale * scale))
    left = lax.broadcasted_iota(jnp.int32, outer.shape, 1) < total
    info = dots((h2, once), (jnp.where(left, h0, h1), twice.astype(BF16)))
    info_ref[:, 0, :] = info[:states, :states]


def shards(state_anom, radiance_anom, inv_noise, innovation, valid_count):
    n_mem, n_chan = lax.axis_size("mem"), lax.axis_size("chan")
    members, states = state_anom.shape[1:]
    width = radiance_anom.shape[2]
    total = members * n_mem
    in_members = total <= states and 2 * total == LANES
    columns = LANES if in_members else total
    height = total * total // columns
    vmem, far = pl.BlockSpec(memory_space=pltpu.VMEM), pl.BlockSpec(memory_space=pltpu.HBM)
    dma = pltpu.SemaphoreType.DMA
    factor = () if not in_members else (jax.ShapeDtypeStruct((total, LANES), F32),
                                        jax.ShapeDtypeStruct((2 * total, 2 * LANES), F32),
                                        jax.ShapeDtypeStruct((total, up(states, LANES)), F32))
    valid_count, state_anom, radiance_anom, inv_noise, innovation = (pltpu.with_memory_space_constraint(x, pltpu.HBM) for x in (valid_count, state_anom, radiance_anom, inv_noise, innovation))
    gram, own_states, *factors = pl.pallas_call(
        functools.partial(gram_kernel, n_mem, n_chan, PARTS),
        out_shape=(jax.ShapeDtypeStruct((height + SUB, columns), F32),
                   jax.ShapeDtypeStruct((n_mem, members, states), BF16)) + factor,
        in_specs=[far] * 5,
        out_specs=(vmem,) * (2 + len(factor)),
        scratch_shapes=[
            pltpu.SMEM(valid_count.shape, jnp.int32),
            pltpu.VMEM((n_mem, members, width), BF16),
            pltpu.VMEM((n_mem, members, states), BF16),
            pltpu.VMEM((width,), F32),
            pltpu.VMEM(innovation.shape, F32),
            pltpu.VMEM((n_mem, members, width), BF16),
            pltpu.VMEM((n_mem, members, states), BF16),
            pltpu.VMEM((n_chan, height + SUB, columns), F32),
            dma((5,)), dma((PARTS, 2)), dma((2,)), dma((max(n_mem // 2 // n_chan, 1), 2)), dma((2,)), dma((2,)),
        ],
        compiler_params=pltpu.CompilerParams(
            collective_id=0, has_side_effects=True, vmem_limit_bytes=24 * MIB),
    )(valid_count, state_anom, radiance_anom, inv_noise, innovation)
    information, gradient, increment = pl.pallas_call(
        functools.partial(solve_in_members if in_members else solve_in_states, total),
        out_shape=(jax.ShapeDtypeStruct((states, 1, states), F32),
                   jax.ShapeDtypeStruct((1, states), F32),
                   jax.ShapeDtypeStruct((1, states), F32)),
        in_specs=[vmem] * (2 + len(factor)),
        out_specs=(vmem, vmem, vmem),
        compiler_params=pltpu.CompilerParams(vmem_limit_bytes=24 * MIB),
    )(gram, own_states, *factors)
    return information.transpose(1, 0, 2), gradient, increment


def solution(mesh):
    in_specs = (P(None, "mem", None), P(None, "mem", "chan"), P("chan"), P(None, "chan"), P())
    out_specs = (P("mem", None, None), P("mem", None), P("mem", None))
    return jax.shard_map(shards, mesh=mesh, in_specs=in_specs, out_specs=out_specs, check_vma=False)
```
